32 devices in a mesh: dp: 8 (over z, y), feat: 4 (over x, core).
Axes of the slice: x: 2, y: 2, z: 4, core: 2. Of those that a mesh axis runs over, the one named last changes fastest.
Arguments:
- observations: bfloat16 [1024, 128, 128], P('dp', 'feat'), may hold values from -1.5 to 1.5
- labels: int32 [1024, 128], P('dp'), may hold values 0 or 1
- tile_live: int32 [1024], P('dp'), may hold values from 1 to 128
- tile_group: int32 [1024], P('dp'), may hold values from 0 to 127, as said below
- position: float32 [128, 2048], P('dp', 'feat'), may hold values from -2.4 to 2.4
- momentum: float32 [128, 2048], P('dp', 'feat'), may hold values from -6 to 6
- gradient: float32 [128, 2048], P('dp', 'feat'), may hold values from -18 to 18
- prior_mean: float32 [2048], P('feat'), may hold values from -1.8 to 1.8
- prior_prec: float32 [128], P('feat'), may hold values from 0.25 to 4
- inv_mass: float32 [128], P('feat'), may hold values from 0.5 to 2
Outputs:
- new_position: float32 [128, 2048], P('dp', 'feat')
- new_momentum: float32 [128, 2048], P('dp', 'feat')
- new_gradient: float32 [128, 2048], P('dp', 'feat')
- energy: float32 [128, 16], P('dp')
The draws below stay inside these ranges and needn't reach their ends.
Inputs may be any that keep to these rules, and one draw needn't show every extreme that they name: `tile_group`: group g belongs to owner g // 16. Among the 128 tiles of one device at most 32 have groups of any one owner, and one owner has exactly 32 tiles from every device. `tile_live`: the live slots of a tile come first.
All inputs are finite; a program needn't handle non-finite values. No bound on the sum of `labels` on one device may be relied on, other than what follows from the above.
Results may differ from the reference program's by a relative error of at most 0.0041.
Values may be sent and summed in bfloat16 or wider, within the bound.
A program may use at most 64 MiB of HBM per device.

```python
import math
import jax
import jax.numpy as jnp
from jax import lax

F = 128
ROWS = 128
TILE_DEV = 128
GRP_DEV = 16
CHAINS = 16
NTILES = 1024
GROUPS = 128


def draw_tile_group(key, part):
    owners = GROUPS // GRP_DEV
    block_total = NTILES // TILE_DEV
    slot_count = max(2, 2 * TILE_DEV // owners)
    hot_owner = jax.random.randint(jax.random.fold_in(key, 11), (), 0, owners)
    spare_count = (owners - 1) * slot_count

    def one_block(block_index):
        block_key = jax.random.fold_in(jax.random.fold_in(key, 12), block_index)
        pick_key, order_key, local_key = jax.random.split(block_key, 3)
        candidate = jnp.arange(spare_count, dtype=jnp.int32) // slot_count
        candidate = candidate + (candidate >= hot_owner).astype(jnp.int32)
        chosen = jax.random.permutation(pick_key, candidate)[:TILE_DEV - slot_count]
        target = jnp.concatenate([jnp.full((slot_count,), hot_owner, jnp.int32), chosen.astype(jnp.int32)])
        target = jax.random.permutation(order_key, target)
        local_group = jax.random.randint(local_key, (TILE_DEV,), 0, GRP_DEV)
        return (target * GRP_DEV + local_group).astype(jnp.int32)
    return jax.vmap(one_block)(jnp.arange(block_total, dtype=jnp.int32)).reshape(NTILES).astype(jnp.int32)


def set_ends(drawn, rng, smallest, high):
    shape = drawn.shape
    index_at = [jax.random.randint(jax.random.fold_in(rng, axis), (), 0, shape[axis]) for axis in range(len(shape))]
    drawn = drawn.at[tuple(index_at)].set(smallest)
    longest = shape.index(max(shape))
    index_at[longest] = (index_at[longest] + 1) % shape[longest]
    return drawn.at[tuple(index_at)].set(high)


def block_levels(rng, dims, pieces, low, high):
    loudness = 1.0
    for dim, blocks in pieces:
        draws = jax.random.uniform(jax.random.fold_in(jax.random.fold_in(rng, 6), dim), (blocks,), jnp.float32, low / len(pieces), high / len(pieces))
        loudness = loudness * jnp.repeat(jnp.exp(draws), dims[dim] // blocks).reshape((-1,) + (1,) * (len(dims) - 1 - dim))
    return loudness


def noise(own_key, extent, width, most, pieces=(), kind=jnp.bfloat16):
    factor_of = block_levels(own_key, extent, pieces, -0.22, 0.18) if pieces else 1.0
    result = jax.random.normal(own_key, extent, jnp.float32) * width * factor_of
    return jnp.minimum(jnp.maximum(result, -most), most).astype(kind)


def setup_inputs(seed: int = 0) -> dict:
    arg_keys = jax.random.split(jax.random.key(seed), 11)
    observations = noise(arg_keys[0], (NTILES, F, ROWS), 0.25, 1.5, ((0, 8), (1, 4)))
    labels = set_ends((jax.random.randint(arg_keys[1], (NTILES, ROWS), 0, 2) < 1).astype(jnp.int32), jax.random.fold_in(arg_keys[1], 1), 0, 1)
    tile_live = set_ends(jax.random.randint(arg_keys[2], (NTILES,), 1, ROWS + 1), jax.random.fold_in(arg_keys[2], 1), 1, ROWS).astype(jnp.int32)
    tile_group = draw_tile_group(jax.random.fold_in(arg_keys[10], 71), 0)
    position = noise(arg_keys[4], (GROUPS, F * CHAINS), 0.4, 2.4, ((0, 8), (1, 4)), jnp.float32)
    momentum = noise(arg_keys[5], (GROUPS, F * CHAINS), 1.0, 6.0, ((0, 8), (1, 4)), jnp.float32)
    gradient = noise(arg_keys[6], (GROUPS, F * CHAINS), 3.0, 18.0, ((0, 8), (1, 4)), jnp.float32)
    prior_mean = noise(arg_keys[7], (F * CHAINS,), 0.3, 1.8, ((0, 4),), jnp.float32)
    prior_prec = jnp.clip(jnp.exp(math.log(4.0) - 2.7725887 * jax.random.uniform(arg_keys[8], (F,), jnp.float32) ** block_levels(arg_keys[8], (F,), ((0, 4),), -0.2, 0.2)), 0.25, 4.0)
    inv_mass = jnp.clip(jnp.exp(math.log(2.0) - 1.3862944 * jax.random.uniform(arg_keys[9], (F,), jnp.float32) ** block_levels(arg_keys[9], (F,), ((0, 4),), -0.2, 0.2)), 0.5, 2.0)
    return {"observations": observations, "labels": labels, "tile_live": tile_live, "tile_group": tile_group, "position": position, "momentum": momentum, "gradient": gradient, "prior_mean": prior_mean, "prior_prec": prior_prec, "inv_mass": inv_mass}


step_size = 0.1


def tile_terms(blocks, observations, labels, tile_live):
    logits = jnp.einsum("tfc,tfr->tcr", blocks.astype(jnp.float32), observations.astype(jnp.float32), precision=lax.Precision.HIGHEST)
    live_rows = (jnp.arange(observations.shape[2], dtype=jnp.int32)[None, :] < tile_live[:, None])[:, None, :]
    targets = labels.astype(jnp.float32)[:, None, :]
    residual = jnp.where(live_rows, jax.nn.sigmoid(logits) - targets, 0.0).astype(jnp.bfloat16)
    neg_loglik = jnp.sum(jnp.where(live_rows, jax.nn.softplus(logits) - targets * logits, 0.0), axis=2)
    partial_value = jnp.einsum("tfr,tcr->tfc", observations.astype(jnp.float32), residual.astype(jnp.float32), precision=lax.Precision.HIGHEST)
    return partial_value.reshape(partial_value.shape[0], -1), neg_loglik


def reference(observations, labels, tile_live, tile_group, position, momentum, gradient, prior_mean, prior_prec, inv_mass):
    prior_full = jnp.repeat(prior_prec, CHAINS)
    mass_full = jnp.repeat(inv_mass, CHAINS)
    half_momentum = momentum - 0.5 * step_size * gradient
    moved_position = position + step_size * mass_full * half_momentum
    rounded = moved_position.astype(jnp.bfloat16)
    block_total = NTILES // TILE_DEV

    def one_block(running, block_items):
        tile_obs, tile_labels, live_count, groups = block_items
        blocks = rounded[groups].reshape(groups.shape[0], F, CHAINS)
        partial_value, neg_loglik = tile_terms(blocks, tile_obs, tile_labels, live_count)
        return running, (partial_value, neg_loglik)

    block_items = (observations.reshape(block_total, TILE_DEV, F, ROWS), labels.reshape(block_total, TILE_DEV, ROWS), tile_live.reshape(block_total, TILE_DEV), tile_group.reshape(block_total, TILE_DEV))
    running, outputs = lax.scan(one_block, jnp.zeros((), jnp.float32), block_items)
    partials, losses = outputs
    likelihood_grad = jax.ops.segment_sum(partials.reshape(NTILES, F * CHAINS), tile_group, num_segments=GROUPS)
    group_loglik = jax.ops.segment_sum(losses.reshape(NTILES, CHAINS), tile_group, num_segments=GROUPS)
    offset = moved_position - prior_mean
    new_gradient = likelihood_grad + prior_full * offset
    new_momentum = half_momentum - 0.5 * step_size * new_gradient
    quadratic = 0.5 * (prior_full * offset * offset + mass_full * new_momentum * new_momentum)
    energy = group_loglik + jnp.sum(quadratic.reshape(GROUPS, F, CHAINS), axis=1)
    return moved_position, new_momentum, new_gradient, energy
```

```python
import functools
import jax
import jax.numpy as jnp
from jax import lax
from jax.experimental import pallas as pl
from jax.experimental.pallas import tpu as pltpu
from jax.sharding import PartitionSpec as P

step_size = 0.1
LANES = 128
PARTS = 2
CHUNKS = 4
MESH = pl.DeviceIdType.MESH
BF16 = jnp.bfloat16
F32 = jnp.float32


def iota(shape, dim):
    return lax.broadcasted_iota(jnp.int32, shape, dim)


def split(x):
    hi = x.astype(BF16)
    return hi, (x - hi.astype(F32)).astype(BF16)


def nt_dot(a, b):
    return lax.dot_general(a, b, (((1,), (1,)), ((), ())), preferred_element_type=F32)


def kernel(
    n, nf, chains, quarter,
    obs_hbm, lab_hbm, live_hbm, grp_hbm, pos_hbm, mom_hbm, grad_hbm, mean_hbm, prec_hbm, mass_hbm,
    newpos_ref, newmom_ref, newgrad_ref, energy_ref,
    lab_in, live_ref, grp_ref, pos_ref, mom_ref, grad_ref, mean_ref, pair_ref,
    lab_ref, par_ref, obs, perm, wall, half_ref, hot_ref, lhs, mine, pair_send, pair_recv,
    far_send, far_recv, res_own, res_recv, nll_ref, dmat, gsend0, gsend1, grecv0, grecv1, esend, erecv,
    in_sem, w_ssem, w_rsem, p_ssem, p_rsem, f_ssem, f_rsem, r_ssem, r_rsem,
    g_ssem, g_rsem, e_ssem, e_rsem,
):
    me = lax.axis_index("dp")
    feat = lax.axis_index("feat")
    tiles = lab_ref.shape[0]
    own, width = pos_ref.shape
    pack = LANES // quarter
    part_chains = chains // PARTS
    part_width = width // PARTS
    quads = tiles // pack
    qrows = pack * part_chains
    half_quads = quads // 2
    chunk_quads = half_quads // CHUNKS
    chunk_tiles = chunk_quads * pack
    crows = chunk_quads * qrows
    groups = n * own
    bit = feat % 2
    near = feat + 1 - 2 * bit
    far = (feat + nf // 2) % nf

    rails = 2 - n % 2
    levels = n // rails
    level, rail = me // rails, me % rails
    mate = me + 1 - 2 * rail
    first_greeted = jnp.maximum(level - 1, 0) * rails
    heard = jnp.minimum((level + 2) * rails, n)

    sources = [
        (mass_hbm, pair_ref.at[1:2]), (prec_hbm, pair_ref.at[0:1]),
        (mom_hbm, mom_ref), (grad_hbm, grad_ref), (pos_hbm, pos_ref), (mean_hbm, mean_ref),
        (grp_hbm, grp_ref), (live_hbm, live_ref), (lab_hbm, lab_in), (obs_hbm, obs),
    ]
    fetches = [pltpu.make_async_copy(a, b, in_sem.at[i]) for i, (a, b) in enumerate(sources)]
    for f in fetches:
        f.start()

    barrier = pltpu.get_barrier_semaphore()

    def greet(i, carry):
        d = first_greeted + i
        d = d + (d >= me).astype(jnp.int32)
        pl.semaphore_signal(barrier, inc=1, device_id={"dp": d}, device_id_type=MESH)
        return carry

    lax.fori_loop(0, n - 1 - first_greeted, greet, 0)
    for i in range(1, nf):
        pl.semaphore_signal(barrier, inc=1, device_id={"feat": (feat + i) % nf}, device_id_type=MESH)

    spread = (iota((quarter, width), 0) == iota((quarter, width), 1) // chains).astype(F32)
    r, c = iota((width, width), 0), iota((width, width), 1)
    perm[...] = jnp.where(
        (r % chains == c // quarter) & (r // chains == c % quarter), 1.0, 0.0
    ).astype(BF16)
    for f in fetches[:5]:
        f.wait()
    par_ref[...] = jnp.dot(
        pair_ref[...], spread, precision=lax.Precision.HIGHEST, preferred_element_type=F32
    )
    half = mom_ref[...] - 0.5 * step_size * grad_ref[...]
    half_ref[...] = half
    moved = pos_ref[...] + step_size * par_ref[1:2, :] * half
    newpos_ref[...] = moved
    coeff = jnp.dot(moved.astype(BF16), perm[...], preferred_element_type=F32).astype(BF16)

    def block(d):
        return pl.ds(pl.multiple_of(d * own, own), own)

    for h in range(PARTS):
        wall[h, block(me), :] = coeff[:, h * part_width:(h + 1) * part_width]
    pl.semaphore_wait(barrier, heard - 1 + nf - 1)

    def w_copy(h, kind, at, origin, to):
        return pltpu.make_async_remote_copy(
            src_ref=wall.at[h, block(origin)], dst_ref=wall.at[h, block(origin)],
            send_sem=w_ssem.at[h, kind, at], recv_sem=w_rsem.at[h, origin],
            device_id={"dp": to}, device_id_type=MESH,
        )

    def ups(h, origin):
        out = [w_copy(h, 1, origin, origin, me + rails)]
        if rails > 1:
            out.append(w_copy(h, 2, origin, origin, mate + rails))
        return out

    has_up = level < levels - 1

    def send_up(h, origin):
        @pl.when(has_up)
        def _():
            for w in ups(h, origin):
                w.start()

    for h in range(PARTS):
        send_up(h, me)
        if rails > 1:
            w_copy(h, 0, mate, me, mate).start()

        def send_down(d, carry, h=h):
            w_copy(h, 0, d, me, d).start()
            return carry

        lax.fori_loop(0, level * rails, send_down, 0)

    square = iota((tiles, tiles), 0) == iota((tiles, tiles), 1)

    def column(row):
        return jnp.sum(jnp.where(square, row.astype(F32), 0.0), axis=1, keepdims=True)

    for f in fetches[5:9]:
        f.wait()
    hot_ref[...] = (
        iota((tiles, groups), 1).astype(F32) == column(grp_ref[...])
    ).astype(F32).astype(BF16)
    lab_ref[...] = jnp.where(
        iota(lab_ref.shape, 1).astype(F32) < column(live_ref[...]), lab_in[...].astype(F32), -1.0
    )
    nll_ref[...] = jnp.zeros_like(nll_ref)
    fetches[9].wait()

    def relay(i, carry):
        origin = me - (i + 1) * rails
        for h in range(PARTS):
            w_copy(h, 0, me, origin, mate).wait_recv()
            send_up(h, origin)
        return carry

    lax.fori_loop(0, level, relay, 0)

    row_t, lane_t = iota((tiles, LANES), 0), iota((tiles, LANES), 1)
    place = row_t % pack
    keep = lane_t // quarter == place

    def wait_blocks(h):
        def step(d, carry):
            relayed = (d // rails < level) & (d % rails == rail)

            @pl.when((d != me) & jnp.logical_not(relayed))
            def _():
                w_copy(h, 0, me, d, mate).wait_recv()
            return carry

        lax.fori_loop(0, n, step, 0)

    def pick(h):
        picked = jnp.dot(hot_ref[...], wall[h], preferred_element_type=F32)
        for m in range(part_width // LANES):
            x = picked[:, m * LANES:(m + 1) * LANES]
            turned = [x] + [pltpu.roll(x, s * quarter, 1) for s in range(1, pack)]
            for j in range(pack):
                y = turned[0]
                for s in range(1, pack):
                    y = jnp.where((place + pack - j) % pack == s, turned[s], y)
                lhs[pl.ds(h * tiles * part_chains + m * pack + j, tiles, stride=part_chains), :] = (
                    jnp.where(keep, y, 0.0)
                )

    def logits(h, first_quad, dst, base):
        for i in range(chunk_quads):
            q = first_quad + i
            at = h * tiles * part_chains + q * qrows
            a = lhs[pl.ds(pl.multiple_of(at, qrows), qrows), :].astype(BF16)
            dst[pl.ds(pl.multiple_of(base + i * qrows, qrows), qrows), :] = jnp.dot(
                a, obs[q], preferred_element_type=F32
            )

    def rows(u):
        return pl.ds(pl.multiple_of(u * crows, crows), crows)

    def pair_copy(u):
        return pltpu.make_async_remote_copy(
            src_ref=pair_send.at[rows(u)], dst_ref=pair_recv.at[rows(u)],
            send_sem=p_ssem.at[u], recv_sem=p_rsem.at[u],
            device_id={"feat": near}, device_id_type=MESH,
        )

    def far_copy(u):
        return pltpu.make_async_remote_copy(
            src_ref=far_send.at[rows(u)], dst_ref=far_recv.at[rows(u)],
            send_sem=f_ssem.at[u], recv_sem=f_rsem.at[u],
            device_id={"feat": far}, device_id_type=MESH,
        )

    def res_copy(u):
        return pltpu.make_async_remote_copy(
            src_ref=res_own.at[rows(u)], dst_ref=res_recv.at[rows(u)],
            send_sem=r_ssem.at[u], recv_sem=r_rsem.at[u],
            device_id={"feat": near}, device_id_type=MESH,
        )

    def stage_a(h, k):
        u = h * CHUNKS + k
        logits(h, (1 - bit) * half_quads + k * chunk_quads, pair_send, u * crows)
        pair_copy(u).start()
        logits(h, bit * half_quads + k * chunk_quads, mine, u * crows)

    def stage_b(h, k):
        u = h * CHUNKS + k
        pair_copy(u).wait()
        total = mine[rows(u), :] + pair_recv[rows(u), :]
        mine[rows(u), :] = total
        far_send[rows(u), :] = total.astype(BF16)
        far_copy(u).start()

    def loop(first, body):
        def step(k, carry):
            body(k)
            return carry

        lax.fori_loop(first, CHUNKS, step, 0)

    for h in range(PARTS):
        wait_blocks(h)
        pick(h)
        loop(0, lambda k: stage_a(h, k))
        loop(0, lambda k: stage_b(h, k))

    diag = iota((qrows, LANES), 0) // part_chains == iota((qrows, LANES), 1) // quarter

    def grads(h, first_quad, src, base):
        for i in range(chunk_quads):
            q = first_quad + i
            a = src[pl.ds(pl.multiple_of(base + i * qrows, qrows), qrows), :]
            g = jnp.where(diag, nt_dot(a, obs[q]), 0.0)
            for j in range(pack):
                dmat[pl.ds(h * part_chains * tiles + q * pack + j, part_chains, stride=tiles), :] = (
                    g[j * part_chains:(j + 1) * part_chains]
                )

    def stage_c(h, k):
        u = h * CHUNKS + k
        far_copy(u).wait()
        z = mine[rows(u), :] + far_recv[rows(u), :].astype(F32)
        first = pl.multiple_of((bit * half_quads + k * chunk_quads) * pack, chunk_tiles)
        lab = lab_ref[pl.ds(first, chunk_tiles), :]
        lab = jnp.broadcast_to(lab[:, None, :], (chunk_tiles, part_chains, LANES)).reshape(crows, LANES)
        live = lab >= 0.0
        e = jnp.exp(-jnp.abs(z))
        inv = 1.0 / (1.0 + e)
        sig = jnp.where(z >= 0.0, inv, e * inv)
        res_own[rows(u), :] = jnp.where(live, sig - lab, 0.0).astype(BF16)
        res_copy(u).start()
        v = jnp.where(live, jnp.maximum(z, 0.0) + jnp.log1p(e) - lab * z, 0.0)
        s = jnp.sum(v, axis=1, keepdims=True) * (2.0 / nf)
        at = iota((crows, LANES), 0) % part_chains + h * part_chains == iota((crows, LANES), 1)
        s = jnp.where(at, s, 0.0).reshape(chunk_tiles, part_chains, LANES)
        nll_ref[pl.ds(first, chunk_tiles), :] += jnp.sum(s, axis=1)
        grads(h, bit * half_quads + k * chunk_quads, res_own, u * crows)

    def stage_d(h, k):
        u = h * CHUNKS + k
        res_copy(u).wait()
        grads(h, (1 - bit) * half_quads + k * chunk_quads, res_recv, u * crows)

    def stage_cd(h, k):
        stage_c(h, k)
        stage_d(h, k - 1)

    seg_groups = min(groups, LANES)
    lane_g = iota((seg_groups, LANES), 1) // quarter
    blocks = part_width // LANES
    sums = ((gsend0, grecv0), (gsend1, grecv1))

    def stacked(d):
        return jnp.concatenate(split(d), axis=0)

    def segment(gc, h):
        gsend = sums[h][0]
        base = gc * seg_groups
        out = pl.ds(pl.multiple_of(base, seg_groups), seg_groups)
        oh = (iota((seg_groups, tiles), 0) + base == grp_ref[...]).astype(F32).astype(BF16)
        oh = jnp.concatenate([oh, oh], axis=1)
        for m in range(blocks):
            packed = None
            for j in range(0, pack, 2):
                at = (h * part_chains + m * pack + j) * tiles
                rhs = jnp.concatenate(
                    [stacked(dmat[at:at + tiles]), stacked(dmat[at + tiles:at + 2 * tiles])], axis=1
                )
                both = jnp.dot(oh, rhs, preferred_element_type=F32)
                for i in range(2):
                    s = both[:, i * LANES:(i + 1) * LANES]
                    shift = LANES // 2
                    while shift >= quarter:
                        s = s + pltpu.roll(s, shift, 1)
                        shift //= 2
                    packed = s if packed is None else jnp.where(lane_g == j + i, s, packed)
            gsend[out, m * LANES:(m + 1) * LANES] = packed.astype(BF16)
        if h == PARTS - 1:
            hi, lo = split(jnp.dot(oh, stacked(nll_ref[...]), preferred_element_type=F32))
            gsend[out, blocks * LANES:] = (
                hi.astype(F32) + pltpu.roll(lo.astype(F32), chains, 1)
            ).astype(BF16)

    def g_copy(h, to):
        return pltpu.make_async_remote_copy(
            src_ref=sums[h][0].at[block(to)], dst_ref=sums[h][1].at[me],
            send_sem=g_ssem.at[h, to], recv_sem=g_rsem.at[h, me],
            device_id={"dp": to}, device_id_type=MESH,
        )

    def g_from(h, d):
        return pltpu.make_async_remote_copy(
            src_ref=sums[h][0].at[block(d)], dst_ref=sums[h][1].at[d],
            send_sem=g_ssem.at[h, d], recv_sem=g_rsem.at[h, d],
            device_id={"dp": d}, device_id_type=MESH,
        )

    def others(body):
        def step(i, carry):
            body(i + (i >= me).astype(jnp.int32))
            return carry

        lax.fori_loop(0, n - 1, step, 0)

    def send_sums(h):
        def run(gc, carry):
            segment(gc, h)
            return carry

        lax.fori_loop(0, groups // seg_groups, run, 0)
        others(lambda d: g_copy(h, d).start())
        sums[h][1][me] = sums[h][0][block(me), :]

    stage_c(0, 0)
    loop(1, lambda k: stage_cd(0, k))
    for h in range(1, PARTS):
        stage_c(h, 0)
        stage_d(h - 1, CHUNKS - 1)
        send_sums(h - 1)
        loop(1, lambda k: stage_cd(h, k))
    stage_d(PARTS - 1, CHUNKS - 1)
    send_sums(PARTS - 1)

    def total_of(h):
        others(lambda d: g_from(h, d).wait())
        shape = sums[h][1].shape[1:]
        return lax.fori_loop(
            0, n, lambda i, t: t + sums[h][1][i].astype(F32), jnp.zeros(shape, F32)
        )

    def natural(packed, h):
        parts = jnp.concatenate(split(packed), axis=0)
        both = nt_dot(parts, perm[:, h * part_width:(h + 1) * part_width])
        return both[:own] + both[own:]

    def drain(h):
        @pl.when(has_up)
        def _():
            for w in ups(h, me):
                w.wait_send()

            def step(i, carry):
                for w in ups(h, me - (i + 1) * rails):
                    w.wait_send()
                return carry

            lax.fori_loop(0, level, step, 0)

        if rails > 1:
            w_copy(h, 0, mate, me, mate).wait_send()

        def down(d, carry):
            w_copy(h, 0, d, me, d).wait_send()
            return carry

        lax.fori_loop(0, level * rails, down, 0)

    for h in range(PARTS):
        drain(h)
    mean, prec, mass = mean_ref[...], par_ref[0:1, :], par_ref[1:2, :]
    offset = newpos_ref[...] - mean
    lik = prec * offset
    for h in range(PARTS):
        total = total_of(h)
        lik = lik + natural(total[:, :part_width], h)
    loss = total[:, part_width:]
    new_gradient = lik
    new_momentum = half_ref[...] - 0.5 * step_size * new_gradient
    newgrad_ref[...] = new_gradient
    newmom_ref[...] = new_momentum
    quad = 0.5 * (prec * offset * offset + mass * new_momentum * new_momentum)
    q = quad[:, :LANES]
    for m in range(1, width // LANES):
        q = q + quad[:, m * LANES:(m + 1) * LANES]
    shift = LANES // 2
    while shift >= chains:
        q = q + pltpu.roll(q, shift, 1)
        shift //= 2
    loss = loss + pltpu.roll(loss, LANES - chains, 1)
    esend[...] = q + loss

    def e_copy(i):
        return pltpu.make_async_remote_copy(
            src_ref=esend, dst_ref=erecv.at[feat], send_sem=e_ssem.at[i],
            recv_sem=e_rsem.at[i], device_id={"feat": (feat + i) % nf}, device_id_type=MESH,
        )

    for i in range(1, nf):
        e_copy(i).start()
    erecv[feat] = esend[...]
    for i in range(1, nf):
        e_copy(i).wait()
    e = erecv[0]
    for i in range(1, nf):
        e = e + erecv[i]
    energy_ref[...] = e[:, :chains]


def finish(*refs):
    sem = refs[8]
    copies = [pltpu.make_async_copy(refs[i], refs[4 + i], sem.at[i]) for i in range(4)]
    for c in copies:
        c.start()
    for c in copies:
        c.wait()


def body(observations, labels, tile_live, tile_group, position, momentum, gradient, prior_mean, prior_prec, inv_mass):
    n, nf = lax.axis_size("dp"), lax.axis_size("feat")
    tiles, quarter, row_count = observations.shape
    own, width = position.shape
    chains = width // quarter
    pack = LANES // quarter
    half_rows = tiles * chains // 2
    anywhere = pl.BlockSpec(memory_space=pl.ANY)
    units = PARTS * CHUNKS
    dma = pltpu.SemaphoreType.DMA
    block = pltpu.VMEM((own, width), F32)
    results = pl.pallas_call(
        functools.partial(kernel, n, nf, chains, quarter),
        out_shape=(block, block, block, pltpu.VMEM((own, chains), F32)),
        in_specs=[anywhere] * 10,
        out_specs=(pl.BlockSpec(memory_space=pltpu.VMEM),) * 4,
        scratch_shapes=[
            pltpu.VMEM((tiles, row_count), jnp.int32),
            pltpu.VMEM((1, tiles), jnp.int32),
            pltpu.VMEM((1, tiles), jnp.int32),
            pltpu.VMEM((own, width), F32),
            pltpu.VMEM((own, width), F32),
            pltpu.VMEM((own, width), F32),
            pltpu.VMEM((1, width), F32),
            pltpu.VMEM((2, quarter), F32),
            pltpu.VMEM((tiles, row_count), F32),
            pltpu.VMEM((2, width), F32),
            pltpu.VMEM((tiles // pack, LANES, row_count), BF16),
            pltpu.VMEM((width, width), BF16),
            pltpu.VMEM((PARTS, n * own, width // PARTS), BF16),
            pltpu.VMEM((own, width), F32),
            pltpu.VMEM((tiles, n * own), BF16),
            pltpu.VMEM((tiles * chains, LANES), F32),
            pltpu.VMEM((half_rows, row_count), F32),
            pltpu.VMEM((half_rows, row_count), F32),
            pltpu.VMEM((half_rows, row_count), F32),
            pltpu.VMEM((half_rows, row_count), BF16),
            pltpu.VMEM((half_rows, row_count), BF16),
            pltpu.VMEM((half_rows, row_count), BF16),
            pltpu.VMEM((half_rows, row_count), BF16),
            pltpu.VMEM((tiles, LANES), F32),
            pltpu.VMEM((chains * tiles, LANES), F32),
            pltpu.VMEM((n * own, width // PARTS), BF16),
            pltpu.VMEM((n * own, width // PARTS + LANES), BF16),
            pltpu.VMEM((n, own, width // PARTS), BF16),
            pltpu.VMEM((n, own, width // PARTS + LANES), BF16),
            pltpu.VMEM((own, LANES), F32),
            pltpu.VMEM((nf, own, LANES), F32),
            dma((10,)),
            dma((PARTS, 3, n)), dma((PARTS, n)),
            dma((units,)), dma((units,)),
            dma((units,)), dma((units,)),
            dma((units,)), dma((units,)),
            dma((PARTS, n)), dma((PARTS, n)),
            dma((nf,)), dma((nf,)),
        ],
        compiler_params=pltpu.CompilerParams(collective_id=0, has_side_effects=True),
    )(
        observations.reshape(tiles // pack, LANES, row_count),
        labels, tile_live.reshape(1, tiles), tile_group.reshape(1, tiles),
        position, momentum, gradient,
        prior_mean.reshape(1, width), prior_prec.reshape(1, quarter), inv_mass.reshape(1, quarter),
    )
    return tuple(pl.pallas_call(
        finish,
        out_shape=tuple(jax.ShapeDtypeStruct(x.shape, x.dtype) for x in results),
        in_specs=[pl.BlockSpec(memory_space=pltpu.VMEM)] * 4,
        out_specs=(anywhere,) * 4,
        scratch_shapes=[dma((4,))],
    )(*(pltpu.with_memory_space_constraint(x, pltpu.VMEM) for x in results)))


def solution(mesh):
    placed = (
        P("dp", "feat", None),
        P("dp", None),
        P("dp"),
        P("dp"),
        P("dp", "feat"),
        P("dp", "feat"),
        P("dp", "feat"),
        P("feat"),
        P("feat"),
        P("feat"),
    )
    return jax.shard_map(
        body,
        mesh=mesh,
        in_specs=placed,
        out_specs=(P("dp", "feat"), P("dp", "feat"), P("dp", "feat"), P("dp", None)),
        check_vma=False,
    )
```

```python
import functools
import jax
import jax.numpy as jnp
from jax import lax
from jax.experimental import pallas as pl
from jax.experimental.pallas import tpu as pltpu
from jax.sharding import PartitionSpec as P

step_size = 0.1
LANES = 128
PARTS = 2
CHUNKS = 4
MESH = pl.DeviceIdType.MESH
BF16 = jnp.bfloat16
F32 = jnp.float32


def iota(shape, dim):
    return lax.broadcasted_iota(jnp.int32, shape, dim)


def split(x):
    hi = x.astype(BF16)
    return hi, (x - hi.astype(F32)).astype(BF16)


def nt_dot(a, b):
    return lax.dot_general(a, b, (((1,), (1,)), ((), ())), preferred_element_type=F32)


def kernel(
    n, nf, chains, quarter,
    obs_hbm, lab_hbm, live_hbm, grp_hbm, pos_hbm, mom_hbm, grad_hbm, mean_hbm, prec_hbm, mass_hbm,
    newpos_ref, newmom_ref, newgrad_ref, energy_ref,
    lab_in, live_ref, grp_ref, pos_ref, mom_ref, grad_ref, mean_ref, pair_ref,
    lab_ref, par_ref, obs, perm, wall, half_ref, hot_ref, sum_ref, lhs, mine, pair_send, pair_recv,
    far_send, far_recv, res_own, res_recv, nll_ref, dmat, acc, gsend0, gsend1, grecv0, grecv1, esend, erecv,
    in_sem, w_ssem, w_rsem, p_ssem, p_rsem, f_ssem, f_rsem, r_ssem, r_rsem,
    g_ssem, g_rsem, e_ssem, e_rsem,
):
    me = lax.axis_index("dp")
    feat = lax.axis_index("feat")
    tiles = lab_ref.shape[0]
    own, width = pos_ref.shape
    pack = LANES // quarter
    part_chains = chains // PARTS
    part_width = width // PARTS
    quads = tiles // pack
    qrows = pack * part_chains
    half_quads = quads // 2
    chunk_quads = half_quads // CHUNKS
    chunk_tiles = chunk_quads * pack
    crows = chunk_quads * qrows
    groups = n * own
    bit = feat % 2
    near = feat + 1 - 2 * bit
    far = (feat + nf // 2) % nf

    barrier = pltpu.get_barrier_semaphore()

    def others(body):
        def up(i, carry):
            body(n - 1 - i)
            return carry

        def down(d, carry):
            body(d)
            return carry

        lax.fori_loop(0, n - 1 - me, up, 0)
        lax.fori_loop(0, me, down, 0)

    def greet(d):
        pl.semaphore_signal(barrier, inc=1, device_id={"dp": d}, device_id_type=MESH)

    others(greet)
    for i in range(1, nf):
        pl.semaphore_signal(barrier, inc=1, device_id={"feat": (feat + i) % nf}, device_id_type=MESH)

    sources = [
        (mass_hbm, pair_ref.at[1:2]), (prec_hbm, pair_ref.at[0:1]),
        (mom_hbm, mom_ref), (grad_hbm, grad_ref), (pos_hbm, pos_ref), (mean_hbm, mean_ref),
        (grp_hbm, grp_ref), (live_hbm, live_ref), (lab_hbm, lab_in), (obs_hbm, obs),
    ]
    fetches = [pltpu.make_async_copy(a, b, in_sem.at[i]) for i, (a, b) in enumerate(sources)]
    for f in fetches:
        f.start()

    spread = (iota((quarter, width), 0) == iota((quarter, width), 1) // chains).astype(F32)
    r, c = iota((width, width), 0), iota((width, width), 1)
    perm[...] = jnp.where(
        (r % chains == c // quarter) & (r // chains == c % quarter), 1.0, 0.0
    ).astype(BF16)
    for f in fetches[:5]:
        f.wait()
    par_ref[...] = jnp.dot(
        pair_ref[...], spread, precision=lax.Precision.HIGHEST, preferred_element_type=F32
    )
    half = mom_ref[...] - 0.5 * step_size * grad_ref[...]
    half_ref[...] = half
    moved = pos_ref[...] + step_size * par_ref[1:2, :] * half
    newpos_ref[...] = moved
    coeff = jnp.dot(moved.astype(BF16), perm[...], preferred_element_type=F32).astype(BF16)

    def block(d):
        return pl.ds(pl.multiple_of(d * own, own), own)

    for h in range(PARTS):
        wall[h, block(me), :] = coeff[:, h * part_width:(h + 1) * part_width]
    pl.semaphore_wait(barrier, n - 1 + nf - 1)

    def w_copy(h, to):
        return pltpu.make_async_remote_copy(
            src_ref=wall.at[h, block(me)], dst_ref=wall.at[h, block(me)],
            send_sem=w_ssem.at[h], recv_sem=w_rsem.at[h],
            device_id={"dp": to}, device_id_type=MESH,
        )

    def w_all(h):
        blocks = wall.at[h, pl.ds(0, (n - 1) * own)]
        return pltpu.make_async_remote_copy(
            src_ref=blocks, dst_ref=blocks, send_sem=w_ssem.at[h], recv_sem=w_rsem.at[h],
            device_id={"dp": (me + 1) % n}, device_id_type=MESH,
        )

    for h in range(PARTS):
        others(lambda d: w_copy(h, d).start())

    square = iota((tiles, tiles), 0) == iota((tiles, tiles), 1)

    def column(row):
        return jnp.sum(jnp.where(square, row.astype(F32), 0.0), axis=1, keepdims=True)

    for f in fetches[5:9]:
        f.wait()
    hot_ref[...] = (
        iota((tiles, groups), 1).astype(F32) == column(grp_ref[...])
    ).astype(F32).astype(BF16)
    member = (iota((groups, tiles), 0) == grp_ref[...]).astype(F32).astype(BF16)
    for i in range(2):
        side = member[:, i * (tiles // 2):(i + 1) * (tiles // 2)]
        sum_ref[i] = jnp.concatenate([side, side], axis=1)
    lab_ref[...] = jnp.where(
        iota(lab_ref.shape, 1).astype(F32) < column(live_ref[...]), lab_in[...].astype(F32), -1.0
    )
    nll_ref[...] = jnp.zeros_like(nll_ref)
    fetches[9].wait()

    half_tiles = tiles // 2
    row_t, lane_t = iota((half_tiles, LANES), 0), iota((half_tiles, LANES), 1)
    place = row_t % pack
    keep = lane_t // quarter == place
    mine_first, near_first = bit * half_tiles, (1 - bit) * half_tiles

    def pick(h, first):
        picked = jnp.dot(
            hot_ref[pl.ds(pl.multiple_of(first, half_tiles), half_tiles), :], wall[h],
            preferred_element_type=F32,
        )
        for m in range(part_width // LANES):
            x = picked[:, m * LANES:(m + 1) * LANES]
            turned = [x] + [pltpu.roll(x, s * quarter, 1) for s in range(1, pack)]
            for j in range(pack):
                y = turned[0]
                for s in range(1, pack):
                    y = jnp.where((place + pack - j) % pack == s, turned[s], y)
                at = (h * tiles + first) * part_chains + m * pack + j
                lhs[pl.ds(at, half_tiles, stride=part_chains), :] = jnp.where(keep, y, 0.0)

    def logits(h, first_quad, dst, base):
        for i in range(chunk_quads):
            q = first_quad + i
            at = h * tiles * part_chains + q * qrows
            a = lhs[pl.ds(pl.multiple_of(at, qrows), qrows), :].astype(BF16)
            dst[base + i * qrows:base + (i + 1) * qrows, :] = jnp.dot(
                a, obs[q], preferred_element_type=F32
            ).astype(dst.dtype)

    units = PARTS * CHUNKS

    def rows(u):
        return pl.ds(u * crows, crows)

    def exchange(src, dst, ssem, rsem, to):
        def copy(u):
            return pltpu.make_async_remote_copy(
                src_ref=src.at[rows(u)], dst_ref=dst.at[rows(u)], send_sem=ssem.at[0],
                recv_sem=rsem.at[u], device_id={"feat": to}, device_id_type=MESH,
            )

        def drain():
            pltpu.make_async_remote_copy(
                src_ref=src, dst_ref=dst, send_sem=ssem.at[0], recv_sem=rsem.at[0],
                device_id={"feat": to}, device_id_type=MESH,
            ).wait_send()

        return copy, drain

    pair_copy, pair_drain = exchange(pair_send, pair_recv, p_ssem, p_rsem, near)
    far_copy, far_drain = exchange(far_send, far_recv, f_ssem, f_rsem, far)
    res_copy, res_drain = exchange(res_own, res_recv, r_ssem, r_rsem, near)

    for h in range(PARTS):
        w_all(h).wait_recv()
        pick(h, near_first)
        for k in range(CHUNKS):
            u = h * CHUNKS + k
            logits(h, (1 - bit) * half_quads + k * chunk_quads, pair_send, u * crows)
            pair_copy(u).start()
        pick(h, mine_first)
        for k in range(CHUNKS):
            u = h * CHUNKS + k
            logits(h, bit * half_quads + k * chunk_quads, mine, u * crows)
        for k in range(CHUNKS):
            u = h * CHUNKS + k
            pair_copy(u).wait_recv()
            total = mine[rows(u), :] + pair_recv[rows(u), :].astype(F32)
            mine[rows(u), :] = total
            far_send[rows(u), :] = total.astype(BF16)
            far_copy(u).start()

    diag = iota((qrows, LANES), 0) // part_chains == iota((qrows, LANES), 1) // quarter

    def grads(h, first_quad, src, base):
        for i in range(chunk_quads):
            q = first_quad + i
            g = jnp.where(diag, nt_dot(src[base + i * qrows:base + (i + 1) * qrows, :], obs[q]), 0.0)
            for j in range(pack):
                dmat[pl.ds(h * part_chains * tiles + q * pack + j, part_chains, stride=tiles), :] = (
                    g[j * part_chains:(j + 1) * part_chains]
                )

    def stage_c(h, k):
        u = h * CHUNKS + k
        far_copy(u).wait_recv()
        z = mine[rows(u), :] + far_recv[rows(u), :].astype(F32)
        first = pl.multiple_of((bit * half_quads + k * chunk_quads) * pack, chunk_tiles)
        lab = lab_ref[pl.ds(first, chunk_tiles), :]
        lab = jnp.broadcast_to(lab[:, None, :], (chunk_tiles, part_chains, LANES)).reshape(crows, LANES)
        live = lab >= 0.0
        e = jnp.exp(-jnp.abs(z))
        inv = 1.0 / (1.0 + e)
        sig = jnp.where(z >= 0.0, inv, e * inv)
        res_own[rows(u), :] = jnp.where(live, sig - lab, 0.0).astype(BF16)
        res_copy(u).start()
        v = jnp.where(live, jnp.maximum(z, 0.0) + jnp.log(1.0 + e) - lab * z, 0.0)
        s = jnp.sum(v, axis=1, keepdims=True) * (2.0 / nf)
        at = iota((crows, LANES), 0) % part_chains + h * part_chains == iota((crows, LANES), 1)
        s = jnp.where(at, s, 0.0).reshape(chunk_tiles, part_chains, LANES)
        nll_ref[pl.ds(first, chunk_tiles), :] += jnp.sum(s, axis=1)
        grads(h, bit * half_quads + k * chunk_quads, res_own, u * crows)

    def stage_d(h, k):
        u = h * CHUNKS + k
        res_copy(u).wait_recv()
        grads(h, (1 - bit) * half_quads + k * chunk_quads, res_recv, u * crows)

    seg_groups = min(groups, LANES)
    lane_g = iota((seg_groups, LANES), 1) // quarter
    blocks = part_width // LANES
    sums = ((gsend0, grecv0), (gsend1, grecv1))

    def stacked(d):
        return jnp.concatenate(split(d), axis=0)

    def segment(gc, h, first, last):
        gsend = sums[h][0]
        base = gc * seg_groups
        out = pl.ds(pl.multiple_of(base, seg_groups), seg_groups)
        oh = sum_ref[first // half_tiles, out, :]
        for m in range(blocks):
            packed = None
            for j in range(0, pack, 2):
                pair = []
                for i in range(2):
                    at = (h * part_chains + m * pack + j + i) * tiles + first
                    pair.append(stacked(dmat[pl.ds(pl.multiple_of(at, half_tiles), half_tiles), :]))
                both = jnp.dot(oh, jnp.concatenate(pair, axis=1), preferred_element_type=F32)
                for i in range(2):
                    s = both[:, i * LANES:(i + 1) * LANES]
                    shift = LANES // 2
                    while shift >= quarter:
                        s = s + pltpu.roll(s, shift, 1)
                        shift //= 2
                    packed = s if packed is None else jnp.where(lane_g == j + i, s, packed)
            cols = slice(m * LANES, (m + 1) * LANES)
            if last:
                gsend[out, cols] = (acc[out, cols] + packed).astype(BF16)
            else:
                acc[out, cols] = packed
        if h == PARTS - 1 and not last:
            mine_nll = nll_ref[pl.ds(pl.multiple_of(first, half_tiles), half_tiles), :]
            hi, lo = split(jnp.dot(oh, stacked(mine_nll), preferred_element_type=F32))
            gsend[out, blocks * LANES:] = (
                hi.astype(F32) + pltpu.roll(lo.astype(F32), chains, 1)
            ).astype(BF16)

    def add_half(h, first, last):
        def run(gc, carry):
            segment(gc, h, first, last)
            return carry

        lax.fori_loop(0, groups // seg_groups, run, 0)

    def g_copy(h, to):
        return pltpu.make_async_remote_copy(
            src_ref=sums[h][0].at[block(to)], dst_ref=sums[h][1].at[me],
            send_sem=g_ssem.at[h], recv_sem=g_rsem.at[h],
            device_id={"dp": to}, device_id_type=MESH,
        )

    def g_all(h):
        return pltpu.make_async_remote_copy(
            src_ref=sums[h][1].at[pl.ds(0, n - 1)], dst_ref=sums[h][1].at[pl.ds(0, n - 1)],
            send_sem=g_ssem.at[h], recv_sem=g_rsem.at[h],
            device_id={"dp": (me + 1) % n}, device_id_type=MESH,
        )

    def send_sums(h):
        others(lambda d: g_copy(h, d).start())
        sums[h][1][me] = sums[h][0][block(me), :]

    for h in range(PARTS):
        for k in range(CHUNKS):
            stage_c(h, k)
            if k:
                stage_d(h, k - 1)
            elif h:
                stage_d(h - 1, CHUNKS - 1)
                add_half(h - 1, near_first, True)
                send_sums(h - 1)
        add_half(h, mine_first, False)
    stage_d(PARTS - 1, CHUNKS - 1)
    add_half(PARTS - 1, near_first, True)
    send_sums(PARTS - 1)

    def total_of(h):
        g_all(h).wait_recv()
        shape = sums[h][1].shape[1:]
        return lax.fori_loop(
            0, n, lambda i, t: t + sums[h][1][i].astype(F32), jnp.zeros(shape, F32)
        )

    def natural(packed, h):
        parts = jnp.concatenate(split(packed), axis=0)
        both = nt_dot(parts, perm[:, h * part_width:(h + 1) * part_width])
        return both[:own] + both[own:]

    mean, prec, mass = mean_ref[...], par_ref[0:1, :], par_ref[1:2, :]
    offset = newpos_ref[...] - mean
    lik = prec * offset
    for h in range(PARTS):
        total = total_of(h)
        lik = lik + natural(total[:, :part_width], h)
    loss = total[:, part_width:]
    new_gradient = lik
    new_momentum = half_ref[...] - 0.5 * step_size * new_gradient
    newgrad_ref[...] = new_gradient
    newmom_ref[...] = new_momentum
    quad = 0.5 * (prec * offset * offset + mass * new_momentum * new_momentum)
    q = quad[:, :LANES]
    for m in range(1, width // LANES):
        q = q + quad[:, m * LANES:(m + 1) * LANES]
    shift = LANES // 2
    while shift >= chains:
        q = q + pltpu.roll(q, shift, 1)
        shift //= 2
    loss = loss + pltpu.roll(loss, LANES - chains, 1)
    esend[...] = q + loss

    def e_copy(i):
        return pltpu.make_async_remote_copy(
            src_ref=esend, dst_ref=erecv.at[feat], send_sem=e_ssem.at[0],
            recv_sem=e_rsem.at[0], device_id={"feat": (feat + i) % nf}, device_id_type=MESH,
        )

    for i in range(1, nf):
        e_copy(i).start()
    erecv[feat] = esend[...]
    for drain in (pair_drain, far_drain, res_drain):
        drain()
    for h in range(PARTS):
        w_all(h).wait_send()
        g_all(h).wait_send()
    pltpu.make_async_remote_copy(
        src_ref=erecv.at[pl.ds(0, nf - 1)], dst_ref=erecv.at[pl.ds(0, nf - 1)],
        send_sem=e_ssem.at[0], recv_sem=e_rsem.at[0],
        device_id={"feat": near}, device_id_type=MESH,
    ).wait()
    e = erecv[0]
    for i in range(1, nf):
        e = e + erecv[i]
    energy_ref[...] = e[:, :chains]


def finish(*refs):
    sem = refs[8]
    copies = [pltpu.make_async_copy(refs[i], refs[4 + i], sem.at[i]) for i in range(4)]
    for c in copies:
        c.start()
    for c in copies:
        c.wait()


def body(observations, labels, tile_live, tile_group, position, momentum, gradient, prior_mean, prior_prec, inv_mass):
    n, nf = lax.axis_size("dp"), lax.axis_size("feat")
    tiles, quarter, row_count = observations.shape
    own, width = position.shape
    chains = width // quarter
    pack = LANES // quarter
    half_rows = tiles * chains // 2
    anywhere = pl.BlockSpec(memory_space=pl.ANY)
    units = PARTS * CHUNKS
    dma = pltpu.SemaphoreType.DMA
    block = pltpu.VMEM((own, width), F32)
    results = pl.pallas_call(
        functools.partial(kernel, n, nf, chains, quarter),
        out_shape=(block, block, block, pltpu.VMEM((own, chains), F32)),
        in_specs=[anywhere] * 10,
        out_specs=(pl.BlockSpec(memory_space=pltpu.VMEM),) * 4,
        scratch_shapes=[
            pltpu.VMEM((tiles, row_count), jnp.int32),
            pltpu.VMEM((1, tiles), jnp.int32),
            pltpu.VMEM((1, tiles), jnp.int32),
            pltpu.VMEM((own, width), F32),
            pltpu.VMEM((own, width), F32),
            pltpu.VMEM((own, width), F32),
            pltpu.VMEM((1, width), F32),
            pltpu.VMEM((2, quarter), F32),
            pltpu.VMEM((tiles, row_count), F32),
            pltpu.VMEM((2, width), F32),
            pltpu.VMEM((tiles // pack, LANES, row_count), BF16),
            pltpu.VMEM((width, width), BF16),
            pltpu.VMEM((PARTS, n * own, width // PARTS), BF16),
            pltpu.VMEM((own, width), F32),
            pltpu.VMEM((tiles, n * own), BF16),
            pltpu.VMEM((2, n * own, tiles), BF16),
            pltpu.VMEM((tiles * chains, LANES), F32),
            pltpu.VMEM((half_rows, row_count), F32),
            pltpu.VMEM((half_rows, row_count), F32),
            pltpu.VMEM((half_rows, row_count), F32),
            pltpu.VMEM((half_rows, row_count), BF16),
            pltpu.VMEM((half_rows, row_count), BF16),
            pltpu.VMEM((half_rows, row_count), BF16),
            pltpu.VMEM((half_rows, row_count), BF16),
            pltpu.VMEM((tiles, LANES), F32),
            pltpu.VMEM((chains * tiles, LANES), F32),
            pltpu.VMEM((n * own, width // PARTS), F32),
            pltpu.VMEM((n * own, width // PARTS), BF16),
            pltpu.VMEM((n * own, width // PARTS + LANES), BF16),
            pltpu.VMEM((n, own, width // PARTS), BF16),
            pltpu.VMEM((n, own, width // PARTS + LANES), BF16),
            pltpu.VMEM((own, LANES), F32),
            pltpu.VMEM((nf, own, LANES), F32),
            dma((10,)),
            dma((PARTS,)), dma((PARTS,)),
            dma((1,)), dma((units,)),
            dma((1,)), dma((units,)),
            dma((1,)), dma((units,)),
            dma((PARTS,)), dma((PARTS,)),
            dma((1,)), dma((1,)),
        ],
        compiler_params=pltpu.CompilerParams(collective_id=0, has_side_effects=True),
    )(
        observations.reshape(tiles // pack, LANES, row_count),
        labels, tile_live.reshape(1, tiles), tile_group.reshape(1, tiles),
        position, momentum, gradient,
        prior_mean.reshape(1, width), prior_prec.reshape(1, quarter), inv_mass.reshape(1, quarter),
    )
    return tuple(pl.pallas_call(
        finish,
        out_shape=tuple(jax.ShapeDtypeStruct(x.shape, x.dtype) for x in results),
        in_specs=[pl.BlockSpec(memory_space=pltpu.VMEM)] * 4,
        out_specs=(anywhere,) * 4,
        scratch_shapes=[dma((4,))],
    )(*(pltpu.with_memory_space_constraint(x, pltpu.VMEM) for x in results)))


def solution(mesh):
    placed = (
        P("dp", "feat", None),
        P("dp", None),
        P("dp"),
        P("dp"),
        P("dp", "feat"),
        P("dp", "feat"),
        P("dp", "feat"),
        P("feat"),
        P("feat"),
        P("feat"),
    )
    return jax.shard_map(
        body,
        mesh=mesh,
        in_specs=placed,
        out_specs=(P("dp", "feat"), P("dp", "feat"), P("dp", "feat"), P("dp", None)),
        check_vma=False,
    )
```

```python
import functools
import jax
import jax.numpy as jnp
from jax import lax
from jax.experimental import pallas as pl
from jax.experimental.pallas import tpu as pltpu
from jax.sharding import PartitionSpec as P

step_size = 0.1
LANES = 128
PARTS = 2
CHUNKS = 4
MESH = pl.DeviceIdType.MESH
BF16 = jnp.bfloat16
F32 = jnp.float32


def iota(shape, dim):
    return lax.broadcasted_iota(jnp.int32, shape, dim)


def split(x):
    hi = x.astype(BF16)
    return hi, (x - hi.astype(F32)).astype(BF16)


def nt_dot(a, b):
    return lax.dot_general(a, b, (((1,), (1,)), ((), ())), preferred_element_type=F32)


def kernel(
    n, nf, chains, quarter,
    obs_hbm, lab_hbm, live_hbm, grp_hbm, pos_hbm, mom_hbm, grad_hbm, mean_hbm, prec_hbm, mass_hbm,
    newpos_ref, newmom_ref, newgrad_ref, energy_ref,
    lab_in, live_ref, grp_ref, pos_ref, mom_ref, grad_ref, mean_ref, pair_ref,
    lab_ref, par_ref, obs, perm, back, hand, wall, half_ref, hot_ref, sum_ref, lhs, mine, pair_send, pair_recv,
    far_send, far_recv, res_own, res_recv, nll_ref, dmat, acc, gsend0, gsend1, grecv0, grecv1, esend, erecv,
    in_sem, h_ssem, h_rsem, w_ssem, w_rsem, t_sem, p_ssem, p_rsem, f_ssem, f_rsem, r_ssem, r_rsem,
    g_ssem, g_rsem, e_ssem, e_rsem,
):
    me = lax.axis_index("dp")
    feat = lax.axis_index("feat")
    tiles = lab_ref.shape[0]
    own, width = pos_ref.shape
    pack = LANES // quarter
    part_chains = chains // PARTS
    part_width = width // PARTS
    octet = 2 * pack
    orows = octet * part_chains
    half_octets = tiles // octet // 2
    chunk_octets = half_octets // CHUNKS
    chunk_tiles = chunk_octets * octet
    crows = chunk_octets * orows
    groups = n * own
    bit = feat % 2
    near = feat + 1 - 2 * bit
    far = (feat + nf // 2) % nf

    barrier = pltpu.get_barrier_semaphore()

    def above(body):
        def step(i, carry):
            body(n - 1 - i)
            return carry

        lax.fori_loop(0, n - 1 - me, step, 0)

    def below(body):
        def step(d, carry):
            body(d)
            return carry

        lax.fori_loop(0, me, step, 0)

    def others(body):
        above(body)
        below(body)

    def greet(d):
        pl.semaphore_signal(barrier, inc=1, device_id={"dp": d}, device_id_type=MESH)

    leads = bit == 1

    @pl.when(leads)
    def _():
        below(greet)

    above(greet)
    for i in range(1, nf):
        pl.semaphore_signal(barrier, inc=1, device_id={"feat": (feat + i) % nf}, device_id_type=MESH)

    sources = [
        (mass_hbm, pair_ref.at[1:2]), (prec_hbm, pair_ref.at[0:1]),
        (mom_hbm, mom_ref), (grad_hbm, grad_ref), (pos_hbm, pos_ref), (mean_hbm, mean_ref),
        (grp_hbm, grp_ref), (live_hbm, live_ref), (lab_hbm, lab_in), (obs_hbm, obs),
    ]
    fetches = [pltpu.make_async_copy(a, b, in_sem.at[i]) for i, (a, b) in enumerate(sources)]
    for f in fetches:
        f.start()

    spread = (iota((quarter, width), 0) == iota((quarter, width), 1) // chains).astype(F32)
    r, c = iota((width, width), 0), iota((width, width), 1)
    perm[...] = jnp.where(
        (r % chains == c // quarter) & (r // chains == c % quarter), 1.0, 0.0
    ).astype(BF16)
    for f in fetches[:5]:
        f.wait()
    par_ref[...] = jnp.dot(
        pair_ref[...], spread, precision=lax.Precision.HIGHEST, preferred_element_type=F32
    )
    half = mom_ref[...] - 0.5 * step_size * grad_ref[...]
    half_ref[...] = half
    moved = pos_ref[...] + step_size * par_ref[1:2, :] * half
    newpos_ref[...] = moved
    coeff = jnp.dot(moved.astype(BF16), perm[...], preferred_element_type=F32).astype(BF16)

    back[...] = jnp.where(
        (c % chains == r // quarter) & (c // chains == r % quarter), 1.0, 0.0
    ).astype(BF16)

    def block(d):
        return pl.ds(pl.multiple_of(d * own, own), own)

    for h in range(PARTS):
        hand[h] = coeff[:, h * part_width:(h + 1) * part_width]

    for h in range(PARTS):
        wall[0, h, block(me), :] = hand[h]
    pl.semaphore_wait(barrier, me + (n - 1 - me) * bit + nf - 1)

    def remote(src, dst, ssem, rsem, to):
        return pltpu.make_async_remote_copy(
            src_ref=src, dst_ref=dst, send_sem=ssem, recv_sem=rsem,
            device_id=to, device_id_type=MESH,
        )

    def hand_copy(h):
        return remote(
            hand.at[h], wall.at[1, h, block(me)], h_ssem.at[0], h_rsem.at[0], {"feat": near}
        )

    def w_copy(h, to, ssem):
        rows = wall.at[0, h, block(me)]
        return remote(rows, rows, ssem, w_rsem.at[h], {"dp": to})

    def t_copy(h, d, to):
        rows = wall.at[1, h, block(d)]
        return remote(rows, rows, w_ssem.at[1], t_sem.at[h, d], {"dp": to})

    def w_all(h):
        blocks = wall.at[0, h, pl.ds(0, (n - 1) * own)]
        return remote(blocks, blocks, w_ssem.at[0], w_rsem.at[h], {"dp": (me + 1) % n})

    def sent(side):
        blocks = wall.at[side, :, pl.ds(0, (n - 1) * own)]
        return remote(blocks, blocks, w_ssem.at[side], w_rsem.at[0], {"dp": (me + 1) % n})

    def pass_on(h, d):
        return remote(
            wall.at[1, h, block(d)], wall.at[0, h, block(d)], w_ssem.at[1], w_rsem.at[h],
            {"feat": near},
        )

    hand_all = remote(hand, hand, h_ssem.at[0], h_rsem.at[0], {"feat": near})

    @pl.when(jnp.logical_not(leads))
    def _():
        for h in range(PARTS):
            hand_copy(h).start()
        for h in range(PARTS):
            below(lambda d: w_copy(h, d, t_sem.at[h, d]).start())

    def send_both(h, d):
        t_copy(h, me, d).start()
        w_copy(h, d, w_ssem.at[0]).start()

    @pl.when(leads)
    def _():
        for h in range(PARTS):
            below(lambda d: w_copy(h, d, w_ssem.at[0]).start())
        hand_all.wait_recv()
        for h in range(PARTS):
            above(lambda d: send_both(h, d))

    square = iota((tiles, tiles), 0) == iota((tiles, tiles), 1)

    def column(row):
        return jnp.sum(jnp.where(square, row.astype(F32), 0.0), axis=1, keepdims=True)

    for f in fetches[5:9]:
        f.wait()
    hot_ref[...] = (
        iota((tiles, groups), 1).astype(F32) == column(grp_ref[...])
    ).astype(F32).astype(BF16)
    member = (iota((groups, tiles), 0) == grp_ref[...]).astype(F32).astype(BF16)
    for i in range(2):
        side = member[:, i * (tiles // 2):(i + 1) * (tiles // 2)]
        sum_ref[i] = jnp.concatenate([side, side], axis=1)
    lab_ref[...] = jnp.where(
        iota(lab_ref.shape, 1).astype(F32) < column(live_ref[...]), lab_in[...].astype(F32), -1.0
    )
    nll_ref[...] = jnp.zeros_like(nll_ref)
    fetches[9].wait()

    half_tiles = tiles // 2
    row_t, lane_t = iota((tiles, LANES), 0), iota((tiles, LANES), 1)
    place = row_t % pack
    keep = lane_t // quarter == place
    sides = (keep & (row_t % octet < pack), keep & (row_t % octet >= pack))
    mine_first, near_first = bit * half_tiles, (1 - bit) * half_tiles

    def hand_over(h, d):
        t_copy(h, d, d).wait_recv()
        pass_on(h, d).start()

    def relay(h):
        @pl.when(leads)
        def _():
            below(lambda d: hand_over(h, d))

    def pick(h):
        picked = jnp.dot(hot_ref[...], wall[0, h], preferred_element_type=F32)
        for m in range(part_width // LANES):
            x = picked[:, m * LANES:(m + 1) * LANES]
            turned = [x] + [pltpu.roll(x, s * quarter, 1) for s in range(1, pack)]
            spots = []
            for j in range(pack):
                y = turned[0]
                for s in range(1, pack):
                    y = jnp.where((place + pack - j) % pack == s, turned[s], y)
                spots.append(y)
            for j in range(0, pack, 2):
                at = (m * pack + j) * octet
                for i, side in enumerate(sides):
                    two = jnp.concatenate([
                        jnp.where(side, y, 0.0).reshape(tiles // octet, octet, LANES)
                        for y in spots[j:j + 2]
                    ], axis=1)
                    lhs[h, :, at:at + 2 * octet, i * LANES:(i + 1) * LANES] = two.astype(BF16)

    def logits(h, first_octet, dst, base):
        for i in range(chunk_octets):
            o = first_octet + i
            dst[base + i * orows:base + (i + 1) * orows, :] = jnp.dot(
                lhs[h, o], obs[o], preferred_element_type=F32
            ).astype(dst.dtype)

    units = PARTS * CHUNKS

    def rows(u):
        return pl.ds(u * crows, crows)

    def exchange(src, dst, ssem, rsem, to):
        def copy(u):
            at = pl.ds(u * crows, crows)
            return remote(src.at[at], dst.at[at], ssem.at[0], rsem.at[u], {"feat": to})

        def drain():
            pltpu.make_async_remote_copy(
                src_ref=src, dst_ref=dst, send_sem=ssem.at[0], recv_sem=rsem.at[0],
                device_id={"feat": to}, device_id_type=MESH,
            ).wait_send()

        return copy, drain

    pair_copy, pair_drain = exchange(pair_send, pair_recv, p_ssem, p_rsem, near)
    far_copy, far_drain = exchange(far_send, far_recv, f_ssem, f_rsem, far)
    res_copy, res_drain = exchange(res_own, res_recv, r_ssem, r_rsem, near)

    for h in range(PARTS):
        if h == 0:
            relay(h)

        w_all(h).wait_recv()
        pick(h)
        mark = h * CHUNKS
        for k in range(CHUNKS):
            logits(h, (1 - bit) * half_octets + k * chunk_octets, pair_send, (mark + k) * crows)
        for u in range(mark, mark + CHUNKS):
            pair_copy(u).start()
        if h + 1 < PARTS:
            relay(h + 1)
        for k in range(CHUNKS):
            logits(h, bit * half_octets + k * chunk_octets, mine, (mark + k) * crows)
        for u in range(mark, mark + CHUNKS):
            pair_copy(u).wait_recv()
            total = mine[rows(u), :] + pair_recv[rows(u), :].astype(F32)
            mine[rows(u), :] = total
            far_send[rows(u), :] = total.astype(BF16)
            far_copy(u).start()

    spot = iota((orows, LANES), 0) % octet
    diag = tuple(spot == iota((orows, LANES), 1) // quarter + i * pack for i in range(2))

    def grads(h, first_octet, src, base):
        for i in range(chunk_octets):
            o = first_octet + i
            g = nt_dot(src[base + i * orows:base + (i + 1) * orows, :], obs[o])
            g = jnp.where(diag[0], g[:, :LANES], jnp.where(diag[1], g[:, LANES:], 0.0))
            tile = pl.ds(pl.multiple_of(o * octet, octet), octet)
            dmat[h * part_chains:(h + 1) * part_chains, tile, :] = g.reshape(part_chains, octet, LANES)

    def residual(u):
        h, k = divmod(u, CHUNKS)
        z = mine[rows(u), :] + far_recv[rows(u), :].astype(F32)
        first = pl.multiple_of((bit * half_octets + k * chunk_octets) * octet, chunk_tiles)
        lab = lab_ref[pl.ds(first, chunk_tiles), :]
        lab = lab.reshape(chunk_octets, 1, octet, LANES)
        lab = jnp.broadcast_to(lab, (chunk_octets, part_chains, octet, LANES)).reshape(crows, LANES)
        live = lab >= 0.0
        e = jnp.exp(-jnp.abs(z))
        inv = 1.0 / (1.0 + e)
        sig = jnp.where(z >= 0.0, inv, e * inv)
        res_own[rows(u), :] = jnp.where(live, sig - lab, 0.0).astype(BF16)
        res_copy(u).start()
        v = jnp.where(live, jnp.maximum(z, 0.0) + jnp.log(1.0 + e) - lab * z, 0.0)
        s = jnp.sum(v, axis=1, keepdims=True) * (2.0 / nf)
        at = iota((crows, LANES), 0) // octet % part_chains + h * part_chains == iota((crows, LANES), 1)
        s = jnp.where(at, s, 0.0).reshape(chunk_octets, part_chains, octet, LANES)
        nll_ref[pl.ds(first, chunk_tiles), :] += jnp.sum(s, axis=1).reshape(chunk_tiles, LANES)

    def mine_grads(u):
        h, k = divmod(u, CHUNKS)
        grads(h, bit * half_octets + k * chunk_octets, res_own, u * crows)

    def near_grads(u):
        h, k = divmod(u, CHUNKS)
        grads(h, (1 - bit) * half_octets + k * chunk_octets, res_recv, u * crows)

    seg_groups = min(groups, LANES)
    lane_g = iota((half_tiles, LANES), 1) // quarter
    blocks = part_width // LANES
    sums = ((gsend0, grecv0), (gsend1, grecv1))

    def stacked(d):
        return jnp.concatenate(split(d), axis=0)

    def fold(xs, width):
        if len(xs) == 1:
            return xs[0]
        half = len(xs) // 2
        shift = half * width
        low = lane_g % len(xs) < half
        pairs = []
        for a, b in zip(xs[:half], xs[half:]):
            other = jnp.where(low, b, a)
            if len(xs) == pack:
                moved = pltpu.roll(other, shift, 1)
            else:
                moved = jnp.where(
                    low, pltpu.roll(other, LANES - shift, 1), pltpu.roll(other, shift, 1)
                )
            pairs.append(jnp.where(low, a, b) + moved)
        return fold(pairs, width)

    def compact(h, first):
        out = []
        for m in range(blocks):
            xs = []
            for j in range(pack):
                tile = pl.ds(pl.multiple_of(first, half_tiles), half_tiles)
                xs.append(dmat[h * part_chains + m * pack + j, tile, :])
            out.append(fold(xs, quarter))
        return stacked(jnp.concatenate(out, axis=1))

    def over_groups(body):
        def run(gc, carry):
            body(pl.ds(pl.multiple_of(gc * seg_groups, seg_groups), seg_groups))
            return carry

        if groups == seg_groups:
            body(pl.ds(0, groups))
        else:
            lax.fori_loop(0, groups // seg_groups, run, 0)

    def member_dot(side, out, rhs):
        return jnp.dot(sum_ref[side, out, :], rhs, preferred_element_type=F32)

    def start_half(h):
        rhs = compact(h, mine_first)
        nll = None
        if h == PARTS - 1:
            nll = stacked(nll_ref[pl.ds(pl.multiple_of(mine_first, half_tiles), half_tiles), :])

        def body(out):
            acc[out, :] = member_dot(bit, out, rhs)
            if nll is not None:
                hi, lo = split(member_dot(bit, out, nll))
                sums[h][0][out, part_width:] = (
                    hi.astype(F32) + pltpu.roll(lo.astype(F32), chains, 1)
                ).astype(BF16)

        over_groups(body)

    def whole(h):
        rhs = compact(h, mine_first), compact(h, near_first)

        def body(out):
            sums[h][0][out, :part_width] = (
                member_dot(bit, out, rhs[0]) + member_dot(1 - bit, out, rhs[1])
            ).astype(BF16)

        over_groups(body)

    def finish_half(h):
        rhs = compact(h, near_first)

        def body(out):
            sums[h][0][out, :part_width] = (acc[out, :] + member_dot(1 - bit, out, rhs)).astype(BF16)

        over_groups(body)

    def g_copy(h, to):
        return pltpu.make_async_remote_copy(
            src_ref=sums[h][0].at[block(to)], dst_ref=sums[h][1].at[me],
            send_sem=g_ssem.at[h], recv_sem=g_rsem.at[h],
            device_id={"dp": to}, device_id_type=MESH,
        )

    def g_all(h):
        return pltpu.make_async_remote_copy(
            src_ref=sums[h][1].at[pl.ds(0, n - 1)], dst_ref=sums[h][1].at[pl.ds(0, n - 1)],
            send_sem=g_ssem.at[h], recv_sem=g_rsem.at[h],
            device_id={"dp": (me + 1) % n}, device_id_type=MESH,
        )

    def send_sums(h):
        others(lambda d: g_copy(h, d).start())
        sums[h][1][me] = sums[h][0][block(me), :]

    lag = 2
    for u in range(units):
        far_copy(u).wait_recv()
        if u >= lag:
            res_copy(u - lag).wait_recv()
        residual(u)
        mine_grads(u)
        if u >= lag:
            near_grads(u - lag)
            h, k = divmod(u - lag, CHUNKS)
            if k == CHUNKS - 1:
                whole(h)
                send_sums(h)
    for u in range(units - lag, units - 1):
        res_copy(u).wait_recv()
        near_grads(u)
    start_half(PARTS - 1)
    res_copy(units - 1).wait_recv()
    near_grads(units - 1)
    finish_half(PARTS - 1)
    send_sums(PARTS - 1)

    def total_of(h):
        g_all(h).wait_recv()
        return jnp.sum(sums[h][1][...].astype(F32), axis=0)

    def natural(packed, h):
        parts = jnp.concatenate(split(packed), axis=0)
        both = jnp.dot(
            parts, back[h * part_width:(h + 1) * part_width, :], preferred_element_type=F32
        )
        return both[:own] + both[own:]

    mean, prec, mass = mean_ref[...], par_ref[0:1, :], par_ref[1:2, :]
    offset = newpos_ref[...] - mean
    lik = prec * offset
    for h in range(PARTS):
        total = total_of(h)
        lik = lik + natural(total[:, :part_width], h)
    loss = total[:, part_width:]
    new_gradient = lik
    new_momentum = half_ref[...] - 0.5 * step_size * new_gradient
    newgrad_ref[...] = new_gradient
    newmom_ref[...] = new_momentum
    quad = 0.5 * (prec * offset * offset + mass * new_momentum * new_momentum)
    q = quad[:, :LANES]
    for m in range(1, width // LANES):
        q = q + quad[:, m * LANES:(m + 1) * LANES]
    shift = LANES // 2
    while shift >= chains:
        q = q + pltpu.roll(q, shift, 1)
        shift //= 2
    loss = loss + pltpu.roll(loss, LANES - chains, 1)
    esend[...] = q + loss

    def e_copy(i):
        return pltpu.make_async_remote_copy(
            src_ref=esend, dst_ref=erecv.at[feat], send_sem=e_ssem.at[0],
            recv_sem=e_rsem.at[0], device_id={"feat": (feat + i) % nf}, device_id_type=MESH,
        )

    for i in range(1, nf):
        e_copy(i).start()
    erecv[feat] = esend[...]
    for drain in (pair_drain, far_drain, res_drain):
        drain()
    for h in range(PARTS):
        g_all(h).wait_send()

    @pl.when(leads)
    def _():
        for side in range(2):
            sent(side).wait_send()

    @pl.when(jnp.logical_not(leads))
    def _():
        hand_all.wait_send()
        for h in range(PARTS):
            below(lambda d: w_copy(h, d, t_sem.at[h, d]).wait_send())

    pltpu.make_async_remote_copy(
        src_ref=erecv.at[pl.ds(0, nf - 1)], dst_ref=erecv.at[pl.ds(0, nf - 1)],
        send_sem=e_ssem.at[0], recv_sem=e_rsem.at[0],
        device_id={"feat": near}, device_id_type=MESH,
    ).wait()
    e = erecv[0]
    for i in range(1, nf):
        e = e + erecv[i]
    energy_ref[...] = e[:, :chains]


def finish(*refs):
    sem = refs[8]
    copies = [pltpu.make_async_copy(refs[i], refs[4 + i], sem.at[i]) for i in range(4)]
    for c in copies:
        c.start()
    for c in copies:
        c.wait()


def body(observations, labels, tile_live, tile_group, position, momentum, gradient, prior_mean, prior_prec, inv_mass):
    n, nf = lax.axis_size("dp"), lax.axis_size("feat")
    tiles, quarter, row_count = observations.shape
    own, width = position.shape
    chains = width // quarter
    pack = LANES // quarter
    half_rows = tiles * chains // 2
    anywhere = pl.BlockSpec(memory_space=pl.ANY)
    units = PARTS * CHUNKS
    dma = pltpu.SemaphoreType.DMA
    block = pltpu.VMEM((own, width), F32)
    results = pl.pallas_call(
        functools.partial(kernel, n, nf, chains, quarter),
        out_shape=(block, block, block, pltpu.VMEM((own, chains), F32)),
        in_specs=[anywhere] * 10,
        out_specs=(pl.BlockSpec(memory_space=pltpu.VMEM),) * 4,
        scratch_shapes=[
            pltpu.VMEM((tiles, row_count), jnp.int32),
            pltpu.VMEM((1, tiles), jnp.int32),
            pltpu.VMEM((1, tiles), jnp.int32),
            pltpu.VMEM((own, width), F32),
            pltpu.VMEM((own, width), F32),
            pltpu.VMEM((own, width), F32),
            pltpu.VMEM((1, width), F32),
            pltpu.VMEM((2, quarter), F32),
            pltpu.VMEM((tiles, row_count), F32),
            pltpu.VMEM((2, width), F32),
            pltpu.VMEM((tiles // pack // 2, 2 * LANES, row_count), BF16),
            pltpu.VMEM((width, width), BF16),
            pltpu.VMEM((width, width), BF16),
            pltpu.VMEM((PARTS, own, width // PARTS), BF16),
            pltpu.VMEM((2, PARTS, n * own, width // PARTS), BF16),
            pltpu.VMEM((own, width), F32),
            pltpu.VMEM((tiles, n * own), BF16),
            pltpu.VMEM((2, n * own, tiles), BF16),
            pltpu.VMEM((PARTS, tiles // pack // 2, 2 * pack * chains // PARTS, 2 * LANES), BF16),
            pltpu.VMEM((half_rows, row_count), F32),
            pltpu.VMEM((half_rows, row_count), F32),
            pltpu.VMEM((half_rows, row_count), F32),
            pltpu.VMEM((half_rows, row_count), BF16),
            pltpu.VMEM((half_rows, row_count), BF16),
            pltpu.VMEM((half_rows, row_count), BF16),
            pltpu.VMEM((half_rows, row_count), BF16),
            pltpu.VMEM((tiles, LANES), F32),
            pltpu.VMEM((chains, tiles, LANES), F32),
            pltpu.VMEM((n * own, width // PARTS), F32),
            pltpu.VMEM((n * own, width // PARTS), BF16),
            pltpu.VMEM((n * own, width // PARTS + LANES), BF16),
            pltpu.VMEM((n, own, width // PARTS), BF16),
            pltpu.VMEM((n, own, width // PARTS + LANES), BF16),
            pltpu.VMEM((own, LANES), F32),
            pltpu.VMEM((nf, own, LANES), F32),
            dma((10,)),
            dma((1,)), dma((1,)),
            dma((2,)), dma((PARTS,)), dma((PARTS, n)),
            dma((1,)), dma((units,)),
            dma((1,)), dma((units,)),
            dma((1,)), dma((units,)),
            dma((PARTS,)), dma((PARTS,)),
            dma((1,)), dma((1,)),
        ],
        compiler_params=pltpu.CompilerParams(collective_id=0, has_side_effects=True),
    )(
        observations.reshape(tiles // pack // 2, 2 * LANES, row_count),
        labels, tile_live.reshape(1, tiles), tile_group.reshape(1, tiles),
        position, momentum, gradient,
        prior_mean.reshape(1, width), prior_prec.reshape(1, quarter), inv_mass.reshape(1, quarter),
    )
    return tuple(pl.pallas_call(
        finish,
        out_shape=tuple(jax.ShapeDtypeStruct(x.shape, x.dtype) for x in results),
        in_specs=[pl.BlockSpec(memory_space=pltpu.VMEM)] * 4,
        out_specs=(anywhere,) * 4,
        scratch_shapes=[dma((4,))],
    )(*(pltpu.with_memory_space_constraint(x, pltpu.VMEM) for x in results)))


def solution(mesh):
    placed = (
        P("dp", "feat", None),
        P("dp", None),
        P("dp"),
        P("dp"),
        P("dp", "feat"),
        P("dp", "feat"),
        P("dp", "feat"),
        P("feat"),
        P("feat"),
        P("feat"),
    )
    return jax.shard_map(
        body,
        mesh=mesh,
        in_specs=placed,
        out_specs=(P("dp", "feat"), P("dp", "feat"), P("dp", "feat"), P("dp", None)),
        check_vma=False,
    )
```

```python
import functools
import jax
import jax.numpy as jnp
from jax import lax
from jax.experimental import pallas as pl
from jax.experimental.pallas import tpu as pltpu
from jax.sharding import PartitionSpec as P

step_size = 0.1
LANES = 128
PARTS = 2
CHUNKS = 4
MESH = pl.DeviceIdType.MESH
BF16 = jnp.bfloat16
F32 = jnp.float32


def iota(shape, dim):
    return lax.broadcasted_iota(jnp.int32, shape, dim)


def split(x):
    hi = x.astype(BF16)
    return hi, (x - hi.astype(F32)).astype(BF16)


def nt_dot(a, b):
    return lax.dot_general(a, b, (((1,), (1,)), ((), ())), preferred_element_type=F32)


def kernel(
    n, nf, chains, quarter,
    obs_hbm, lab_hbm, live_hbm, grp_hbm, pos_hbm, mom_hbm, grad_hbm, mean_hbm, prec_hbm, mass_hbm,
    newpos_ref, newmom_ref, newgrad_ref, energy_ref,
    lab_in, live_ref, grp_ref, pos_ref, mom_ref, grad_ref, mean_ref, pair_ref,
    lab_ref, par_ref, obs, perm, back, hand, wall, half_ref, drift_ref, lane_mass_ref, gather_ref, e0_ref, hot_ref, sum_ref, lhs, mine, pair_send, pair_recv,
    far_send, far_recv, res_own, res_recv, nll_ref, dmat, acc, gsend0, gsend1, nsend, grecv0, grecv1, nrecv, esend, erecv,
    in_sem, h_rsem, w_rsem, t_sem, p_rsem, f_rsem, g_rsem, e_rsem,
):
    h_ssem, w_ssem, p_ssem, f_ssem = (in_sem.at[i:j] for i, j in ((0, 1), (1, 3), (3, 4), (4, 5)))
    r_ssem, g_ssem, e_ssem = (in_sem.at[i:j] for i, j in ((5, 6), (6, 9), (9, 10)))
    r_rsem = t_sem.at[0]
    me = lax.axis_index("dp")
    feat = lax.axis_index("feat")
    tiles = lab_ref.shape[0]
    own, width = pos_ref.shape
    pack = LANES // quarter
    part_chains = chains // PARTS
    part_width = width // PARTS
    octet = 2 * pack
    orows = octet * part_chains
    half_octets = tiles // octet // 2
    chunk_octets = half_octets // CHUNKS
    chunk_tiles = chunk_octets * octet
    crows = chunk_octets * orows
    groups = n * own
    bit = feat % 2
    near = feat + 1 - 2 * bit
    far = (feat + nf // 2) % nf

    barrier = pltpu.get_barrier_semaphore()

    def above(body):
        def step(i, carry):
            body(n - 1 - i)
            return carry

        lax.fori_loop(0, n - 1 - me, step, 0)

    def below(body):
        def step(d, carry):
            body(d)
            return carry

        lax.fori_loop(0, me, step, 0)

    def others(body):
        above(body)
        below(body)

    def greet(d):
        pl.semaphore_signal(barrier, inc=1, device_id={"dp": d}, device_id_type=MESH)

    leads = bit == 1

    @pl.when(leads)
    def _():
        below(greet)

    above(greet)
    for i in range(1, nf):
        pl.semaphore_signal(barrier, inc=1, device_id={"feat": (feat + i) % nf}, device_id_type=MESH)

    sources = [
        (mass_hbm, pair_ref.at[1:2]), (prec_hbm, pair_ref.at[0:1]),
        (mom_hbm, mom_ref), (grad_hbm, grad_ref), (pos_hbm, pos_ref), (mean_hbm, mean_ref),
        (grp_hbm, grp_ref), (live_hbm, live_ref), (lab_hbm, lab_in), (obs_hbm, obs),
    ]
    fetches = [pltpu.make_async_copy(a, b, in_sem.at[i]) for i, (a, b) in enumerate(sources)]
    for f in fetches:
        f.start()

    spread = (iota((quarter, width), 0) == iota((quarter, width), 1) // chains).astype(F32)
    r, c = iota((width, width), 0), iota((width, width), 1)
    perm[...] = jnp.where(
        (r % chains == c // quarter) & (r // chains == c % quarter), 1.0, 0.0
    ).astype(BF16)
    for f in fetches[:5]:
        f.wait()
    par_ref[...] = jnp.dot(
        pair_ref[...], spread, precision=lax.Precision.HIGHEST, preferred_element_type=F32
    )
    half = mom_ref[...] - 0.5 * step_size * grad_ref[...]
    half_ref[...] = half
    moved = pos_ref[...] + step_size * par_ref[1:2, :] * half
    newpos_ref[...] = moved
    coeff = jnp.dot(moved.astype(BF16), perm[...], preferred_element_type=F32).astype(BF16)

    back[...] = jnp.where(
        (c % chains == r // quarter) & (c // chains == r % quarter), 1.0, 0.0
    ).astype(BF16)

    def block(d):
        return pl.ds(pl.multiple_of(d * own, own), own)

    for h in range(PARTS):
        hand[h] = coeff[:, h * part_width:(h + 1) * part_width]

    for h in range(PARTS):
        wall[0, h, block(me), :] = hand[h]
    pl.semaphore_wait(barrier, me + (n - 1 - me) * bit + nf - 1)

    def remote(src, dst, ssem, rsem, to):
        return pltpu.make_async_remote_copy(
            src_ref=src, dst_ref=dst, send_sem=ssem, recv_sem=rsem,
            device_id=to, device_id_type=MESH,
        )

    def hand_copy(h):
        return remote(
            hand.at[h], wall.at[1, h, block(me)], h_ssem.at[0], h_rsem.at[0], {"feat": near}
        )

    def w_copy(h, to, ssem):
        rows = wall.at[0, h, block(me)]
        return remote(rows, rows, ssem, w_rsem.at[h], {"dp": to})

    def t_copy(h, d, to):
        rows = wall.at[1, h, block(d)]
        return remote(rows, rows, w_ssem.at[1], t_sem.at[h, d], {"dp": to})

    def w_all(h):
        blocks = wall.at[0, h, pl.ds(0, (n - 1) * own)]
        return remote(blocks, blocks, w_ssem.at[0], w_rsem.at[h], {"dp": (me + 1) % n})

    def sent(side):
        blocks = wall.at[side, :, pl.ds(0, (n - 1) * own)]
        return remote(blocks, blocks, w_ssem.at[side], w_rsem.at[0], {"dp": (me + 1) % n})

    def pass_on(h, d):
        return remote(
            wall.at[1, h, block(d)], wall.at[0, h, block(d)], w_ssem.at[1], w_rsem.at[h],
            {"feat": near},
        )

    hand_all = remote(hand, hand, h_ssem.at[0], h_rsem.at[0], {"feat": near})

    @pl.when(jnp.logical_not(leads))
    def _():
        for h in range(PARTS):
            hand_copy(h).start()
        for h in range(PARTS):
            below(lambda d: w_copy(h, d, t_sem.at[h, d]).start())

    def send_both(h, d):
        t_copy(h, me, d).start()
        w_copy(h, d, w_ssem.at[0]).start()

    @pl.when(leads)
    def _():
        for h in range(PARTS):
            below(lambda d: w_copy(h, d, w_ssem.at[0]).start())
        hand_all.wait_recv()
        for h in range(PARTS):
            above(lambda d: send_both(h, d))

    square = iota((tiles, tiles), 0) == iota((tiles, tiles), 1)

    def column(row):
        return jnp.sum(jnp.where(square, row.astype(F32), 0.0), axis=1, keepdims=True)

    for f in fetches[5:9]:
        f.wait()
    hot_ref[...] = (
        iota((tiles, groups), 1).astype(F32) == column(grp_ref[...])
    ).astype(F32).astype(BF16)
    member = (iota((groups, tiles), 0) == grp_ref[...]).astype(F32).astype(BF16)
    for i in range(2):
        side = member[:, i * (tiles // 2):(i + 1) * (tiles // 2)]
        sum_ref[i] = jnp.concatenate([side, side], axis=1)
    lab_ref[...] = jnp.where(
        iota(lab_ref.shape, 1).astype(F32) < column(live_ref[...]), lab_in[...].astype(F32), -1.0
    )
    nll_ref[...] = jnp.zeros_like(nll_ref)
    offset = newpos_ref[...] - mean_ref[...]
    force = par_ref[0:1, :] * offset
    drift = half_ref[...] - 0.5 * step_size * force
    high, rest = split(drift)
    low = (drift - high.astype(F32) - rest.astype(F32)).astype(BF16)
    packed = jnp.dot(
        jnp.concatenate([high, rest, low], axis=0), perm[...], preferred_element_type=F32
    )
    drift_ref[...] = packed[:own] + packed[own:2 * own] + packed[2 * own:]
    lane_mass_ref[...] = jnp.dot(
        pair_ref[...], (iota((quarter, width), 0) == iota((quarter, width), 1) % quarter).astype(F32),
        precision=lax.Precision.HIGHEST, preferred_element_type=F32,
    )[1:2, :]
    gather_ref[...] = (
        iota((width, LANES), 0) // quarter == iota((width, LANES), 1)
    ).astype(F32).astype(BF16)
    prior = 0.5 * force * offset
    e0 = prior[:, :LANES]
    for m in range(1, width // LANES):
        e0 = e0 + prior[:, m * LANES:(m + 1) * LANES]
    shift = LANES // 2
    while shift >= chains:
        e0 = e0 + pltpu.roll(e0, shift, 1)
        shift //= 2
    e0_ref[...] = e0
    fetches[9].wait()

    half_tiles = tiles // 2
    row_t, lane_t = iota((tiles, LANES), 0), iota((tiles, LANES), 1)
    place = row_t % pack
    keep = lane_t // quarter == place
    sides = (keep & (row_t % octet < pack), keep & (row_t % octet >= pack))
    mine_first, near_first = bit * half_tiles, (1 - bit) * half_tiles

    def hand_over(h, d):
        t_copy(h, d, d).wait_recv()
        pass_on(h, d).start()

    def relay(h):
        @pl.when(leads)
        def _():
            below(lambda d: hand_over(h, d))

    def pick(h):
        picked = jnp.dot(hot_ref[...], wall[0, h], preferred_element_type=F32)
        for m in range(part_width // LANES):
            x = picked[:, m * LANES:(m + 1) * LANES]
            turned = [x] + [pltpu.roll(x, s * quarter, 1) for s in range(1, pack)]
            spots = []
            for j in range(pack):
                y = turned[0]
                for s in range(1, pack):
                    y = jnp.where((place + pack - j) % pack == s, turned[s], y)
                spots.append(y)
            for j in range(0, pack, 2):
                at = (m * pack + j) * octet
                for i, side in enumerate(sides):
                    two = jnp.concatenate([
                        jnp.where(side, y, 0.0).reshape(tiles // octet, octet, LANES)
                        for y in spots[j:j + 2]
                    ], axis=1)
                    lhs[h, :, at:at + 2 * octet, i * LANES:(i + 1) * LANES] = two.astype(BF16)

    def logits(h, first_octet, dst, base):
        for i in range(chunk_octets):
            o = first_octet + i
            dst[base + i * orows:base + (i + 1) * orows, :] = jnp.dot(
                lhs[h, o], obs[o], preferred_element_type=F32
            ).astype(dst.dtype)

    units = PARTS * CHUNKS

    def rows(u):
        return pl.ds(u * crows, crows)

    def exchange(src, dst, ssem, rsem, to):
        def copy(u):
            at = pl.ds(u * crows, crows)
            return remote(src.at[at], dst.at[at], ssem.at[0], rsem.at[u], {"feat": to})

        def drain():
            pltpu.make_async_remote_copy(
                src_ref=src, dst_ref=dst, send_sem=ssem.at[0], recv_sem=rsem.at[0],
                device_id={"feat": to}, device_id_type=MESH,
            ).wait_send()

        return copy, drain

    pair_copy, pair_drain = exchange(pair_send, pair_recv, p_ssem, p_rsem, near)
    far_copy, far_drain = exchange(far_send, far_recv, f_ssem, f_rsem, far)
    res_copy, res_drain = exchange(res_own, res_recv, r_ssem, r_rsem, near)

    for h in range(PARTS):
        if h == 0:
            relay(h)

        w_all(h).wait_recv()
        pl.when(jnp.logical_not(leads))(
            lambda: below(lambda d: w_copy(h, d, t_sem.at[h, d]).wait_send())
        )
        pick(h)
        mark = h * CHUNKS
        for k in range(CHUNKS):
            logits(h, (1 - bit) * half_octets + k * chunk_octets, pair_send, (mark + k) * crows)
        for u in range(mark, mark + CHUNKS):
            pair_copy(u).start()
        if h + 1 < PARTS:
            relay(h + 1)
        for k in range(CHUNKS):
            logits(h, bit * half_octets + k * chunk_octets, mine, (mark + k) * crows)
        for u in range(mark, mark + CHUNKS):
            pair_copy(u).wait_recv()
            total = mine[rows(u), :] + pair_recv[rows(u), :].astype(F32)
            mine[rows(u), :] = total
            far_send[rows(u), :] = total.astype(BF16)
            far_copy(u).start()

    spot = iota((orows, LANES), 0) % octet
    diag = tuple(spot == iota((orows, LANES), 1) // quarter + i * pack for i in range(2))

    def grads(h, first_octet, src, base):
        for i in range(chunk_octets):
            o = first_octet + i
            g = nt_dot(src[base + i * orows:base + (i + 1) * orows, :], obs[o])
            g = jnp.where(diag[0], g[:, :LANES], jnp.where(diag[1], g[:, LANES:], 0.0))
            tile = pl.ds(pl.multiple_of(o * octet, octet), octet)
            dmat[h * part_chains:(h + 1) * part_chains, tile, :] = g.reshape(part_chains, octet, LANES)

    def residual(u):
        h, k = divmod(u, CHUNKS)
        z = mine[rows(u), :] + far_recv[rows(u), :].astype(F32)
        first = pl.multiple_of((bit * half_octets + k * chunk_octets) * octet, chunk_tiles)
        lab = lab_ref[pl.ds(first, chunk_tiles), :]
        lab = lab.reshape(chunk_octets, 1, octet, LANES)
        lab = jnp.broadcast_to(lab, (chunk_octets, part_chains, octet, LANES)).reshape(crows, LANES)
        live = lab >= 0.0
        e = jnp.exp(-jnp.abs(z))
        inv = 1.0 / (1.0 + e)
        sig = jnp.where(z >= 0.0, inv, e * inv)
        res_own[rows(u), :] = jnp.where(live, sig - lab, 0.0).astype(BF16)
        res_copy(u).start()
        v = jnp.where(live, jnp.maximum(z, 0.0) + jnp.log(1.0 + e) - lab * z, 0.0)
        s = jnp.sum(v, axis=1, keepdims=True) * (2.0 / nf)
        at = iota((crows, LANES), 0) // octet % part_chains + h * part_chains == iota((crows, LANES), 1)
        s = jnp.where(at, s, 0.0).reshape(chunk_octets, part_chains, octet, LANES)
        nll_ref[pl.ds(first, chunk_tiles), :] += jnp.sum(s, axis=1).reshape(chunk_tiles, LANES)

    def mine_grads(u):
        h, k = divmod(u, CHUNKS)
        grads(h, bit * half_octets + k * chunk_octets, res_own, u * crows)

    def near_grads(u):
        h, k = divmod(u, CHUNKS)
        grads(h, (1 - bit) * half_octets + k * chunk_octets, res_recv, u * crows)

    seg_groups = min(groups, LANES)
    lane_g = iota((half_tiles, LANES), 1) // quarter
    blocks = part_width // LANES
    sums = ((gsend0, grecv0), (gsend1, grecv1), (nsend, nrecv))

    def stacked(d):
        return jnp.concatenate(split(d), axis=0)

    def fold(xs, width):
        if len(xs) == 1:
            return xs[0]
        half = len(xs) // 2
        shift = half * width
        low = lane_g % len(xs) < half
        pairs = []
        for a, b in zip(xs[:half], xs[half:]):
            other = jnp.where(low, b, a)
            if len(xs) == pack:
                moved = pltpu.roll(other, shift, 1)
            else:
                moved = jnp.where(
                    low, pltpu.roll(other, LANES - shift, 1), pltpu.roll(other, shift, 1)
                )
            pairs.append(jnp.where(low, a, b) + moved)
        return fold(pairs, width)

    def compact(h, first):
        out = []
        for m in range(blocks):
            xs = []
            for j in range(pack):
                tile = pl.ds(pl.multiple_of(first, half_tiles), half_tiles)
                xs.append(dmat[h * part_chains + m * pack + j, tile, :])
            out.append(fold(xs, quarter))
        return stacked(jnp.concatenate(out, axis=1))

    def over_groups(body):
        def run(gc, carry):
            body(pl.ds(pl.multiple_of(gc * seg_groups, seg_groups), seg_groups))
            return carry

        if groups == seg_groups:
            body(pl.ds(0, groups))
        else:
            lax.fori_loop(0, groups // seg_groups, run, 0)

    def member_dot(side, out, rhs):
        return jnp.dot(sum_ref[side, out, :], rhs, preferred_element_type=F32)

    def start_half(h):
        rhs = compact(h, mine_first)
        nll = None
        if h == PARTS - 1:
            nll = stacked(nll_ref[pl.ds(pl.multiple_of(mine_first, half_tiles), half_tiles), :])

        def body(out):
            acc[out, :] = member_dot(bit, out, rhs)
            if nll is not None:
                hi, lo = split(member_dot(bit, out, nll))
                nsend[out, :] = (
                    hi.astype(F32) + pltpu.roll(lo.astype(F32), chains, 1)
                ).astype(BF16)

        over_groups(body)

    def whole(h):
        rhs = compact(h, mine_first), compact(h, near_first)

        def body(out):
            sums[h][0][out, :] = (
                member_dot(bit, out, rhs[0]) + member_dot(1 - bit, out, rhs[1])
            ).astype(BF16)

        over_groups(body)

    def finish_half(h):
        rhs = compact(h, near_first)

        def body(out):
            sums[h][0][out, :] = (acc[out, :] + member_dot(1 - bit, out, rhs)).astype(BF16)

        over_groups(body)

    def g_copy(h, to):
        return pltpu.make_async_remote_copy(
            src_ref=sums[h][0].at[block(to)], dst_ref=sums[h][1].at[me],
            send_sem=g_ssem.at[h], recv_sem=g_rsem.at[h],
            device_id={"dp": to}, device_id_type=MESH,
        )

    def g_all(h):
        return pltpu.make_async_remote_copy(
            src_ref=sums[h][1].at[pl.ds(0, n - 1)], dst_ref=sums[h][1].at[pl.ds(0, n - 1)],
            send_sem=g_ssem.at[h], recv_sem=g_rsem.at[h],
            device_id={"dp": (me + 1) % n}, device_id_type=MESH,
        )

    def send_sums(h):
        others(lambda d: g_copy(h, d).start())
        sums[h][1][me] = sums[h][0][block(me), :]

    lag = 2
    for u in range(units):
        far_copy(u).wait_recv()
        if u >= lag:
            res_copy(u - lag).wait_recv()
        residual(u)
        mine_grads(u)
        if u >= lag:
            near_grads(u - lag)
            h, k = divmod(u - lag, CHUNKS)
            if k == CHUNKS - 1:
                whole(h)
                send_sums(h)
    for u in range(units - lag, units - 1):
        res_copy(u).wait_recv()
        near_grads(u)
    start_half(PARTS - 1)
    send_sums(PARTS)
    res_copy(units - 1).wait_recv()
    near_grads(units - 1)
    finish_half(PARTS - 1)
    send_sums(PARTS - 1)

    def total_of(h):
        g_all(h).wait_recv()
        return jnp.sum(sums[h][1][...].astype(F32), axis=0)

    def natural(packed, h):
        parts = jnp.concatenate(split(packed), axis=0)
        both = jnp.dot(
            parts, back[h * part_width:(h + 1) * part_width, :], preferred_element_type=F32
        )
        return both[:own] + both[own:]

    energy = e0_ref[...]
    totals = []
    for h in range(PARTS):
        if h == PARTS - 1:
            loss = total_of(PARTS)
            energy = energy + loss + pltpu.roll(loss, LANES - chains, 1)
        totals.append(total_of(h))
        cols = slice(h * part_width, (h + 1) * part_width)
        t = drift_ref[:, cols] - 0.5 * step_size * totals[h]
        parts = stacked(0.5 * lane_mass_ref[:, cols] * t * t)
        both = jnp.dot(parts, gather_ref[cols, :], preferred_element_type=F32)
        energy = energy + both[:own] + both[own:]
    esend[...] = energy

    def e_copy(i):
        return pltpu.make_async_remote_copy(
            src_ref=esend, dst_ref=erecv.at[feat], send_sem=e_ssem.at[0],
            recv_sem=e_rsem.at[0], device_id={"feat": (feat + i) % nf}, device_id_type=MESH,
        )

    for i in range(1, nf):
        e_copy(i).start()
    erecv[feat] = esend[...]
    new_gradient = par_ref[0:1, :] * (newpos_ref[...] - mean_ref[...])
    for h in range(PARTS):
        new_gradient = new_gradient + natural(totals[h], h)
    newgrad_ref[...] = new_gradient
    newmom_ref[...] = half_ref[...] - 0.5 * step_size * new_gradient
    for drain in (pair_drain, far_drain, res_drain):
        drain()
    for h in range(PARTS + 1):
        g_all(h).wait_send()

    @pl.when(leads)
    def _():
        for side in range(2):
            sent(side).wait_send()

    @pl.when(jnp.logical_not(leads))
    def _():
        hand_all.wait_send()

    pltpu.make_async_remote_copy(
        src_ref=erecv.at[pl.ds(0, nf - 1)], dst_ref=erecv.at[pl.ds(0, nf - 1)],
        send_sem=e_ssem.at[0], recv_sem=e_rsem.at[0],
        device_id={"feat": near}, device_id_type=MESH,
    ).wait()
    e = erecv[0]
    for i in range(1, nf):
        e = e + erecv[i]
    energy_ref[...] = e[:, :chains]


def finish(*refs):
    sem = refs[8]
    copies = [pltpu.make_async_copy(refs[i], refs[4 + i], sem.at[i]) for i in range(4)]
    for c in copies:
        c.start()
    for c in copies:
        c.wait()


def body(observations, labels, tile_live, tile_group, position, momentum, gradient, prior_mean, prior_prec, inv_mass):
    n, nf = lax.axis_size("dp"), lax.axis_size("feat")
    tiles, quarter, row_count = observations.shape
    own, width = position.shape
    chains = width // quarter
    pack = LANES // quarter
    half_rows = tiles * chains // 2
    anywhere = pl.BlockSpec(memory_space=pl.ANY)
    units = PARTS * CHUNKS
    dma = pltpu.SemaphoreType.DMA
    block = pltpu.VMEM((own, width), F32)
    results = pl.pallas_call(
        functools.partial(kernel, n, nf, chains, quarter),
        out_shape=(block, block, block, pltpu.VMEM((own, chains), F32)),
        in_specs=[anywhere] * 10,
        out_specs=(pl.BlockSpec(memory_space=pltpu.VMEM),) * 4,
        scratch_shapes=[
            pltpu.VMEM((tiles, row_count), jnp.int32),
            pltpu.VMEM((1, tiles), jnp.int32),
            pltpu.VMEM((1, tiles), jnp.int32),
            pltpu.VMEM((own, width), F32),
            pltpu.VMEM((own, width), F32),
            pltpu.VMEM((own, width), F32),
            pltpu.VMEM((1, width), F32),
            pltpu.VMEM((2, quarter), F32),
            pltpu.VMEM((tiles, row_count), F32),
            pltpu.VMEM((2, width), F32),
            pltpu.VMEM((tiles // pack // 2, 2 * LANES, row_count), BF16),
            pltpu.VMEM((width, width), BF16),
            pltpu.VMEM((width, width), BF16),
            pltpu.VMEM((PARTS, own, width // PARTS), BF16),
            pltpu.VMEM((2, PARTS, n * own, width // PARTS), BF16),
            pltpu.VMEM((own, width), F32),
            pltpu.VMEM((own, width), F32),
            pltpu.VMEM((1, width), F32),
            pltpu.VMEM((width, LANES), BF16),
            pltpu.VMEM((own, LANES), F32),
            pltpu.VMEM((tiles, n * own), BF16),
            pltpu.VMEM((2, n * own, tiles), BF16),
            pltpu.VMEM((PARTS, tiles // pack // 2, 2 * pack * chains // PARTS, 2 * LANES), BF16),
            pltpu.VMEM((half_rows, row_count), F32),
            pltpu.VMEM((half_rows, row_count), F32),
            pltpu.VMEM((half_rows, row_count), F32),
            pltpu.VMEM((half_rows, row_count), BF16),
            pltpu.VMEM((half_rows, row_count), BF16),
            pltpu.VMEM((half_rows, row_count), BF16),
            pltpu.VMEM((half_rows, row_count), BF16),
            pltpu.VMEM((tiles, LANES), F32),
            pltpu.VMEM((chains, tiles, LANES), F32),
            pltpu.VMEM((n * own, width // PARTS), F32),
            pltpu.VMEM((n * own, width // PARTS), BF16),
            pltpu.VMEM((n * own, width // PARTS), BF16),
            pltpu.VMEM((n * own, LANES), BF16),
            pltpu.VMEM((n, own, width // PARTS), BF16),
            pltpu.VMEM((n, own, width // PARTS), BF16),
            pltpu.VMEM((n, own, LANES), BF16),
            pltpu.VMEM((own, LANES), F32),
            pltpu.VMEM((nf, own, LANES), F32),
            dma((10,)),
            dma((1,)), dma((PARTS,)), dma((PARTS, max(n, units))),
            dma((units,)), dma((units,)), dma((PARTS + 1,)), dma((1,)),
        ],
        compiler_params=pltpu.CompilerParams(collective_id=0, has_side_effects=True),
    )(
        observations.reshape(tiles // pack // 2, 2 * LANES, row_count),
        labels, tile_live.reshape(1, tiles), tile_group.reshape(1, tiles),
        position, momentum, gradient,
        prior_mean.reshape(1, width), prior_prec.reshape(1, quarter), inv_mass.reshape(1, quarter),
    )
    return tuple(pl.pallas_call(
        finish,
        out_shape=tuple(jax.ShapeDtypeStruct(x.shape, x.dtype) for x in results),
        in_specs=[pl.BlockSpec(memory_space=pltpu.VMEM)] * 4,
        out_specs=(anywhere,) * 4,
        scratch_shapes=[dma((4,))],
    )(*(pltpu.with_memory_space_constraint(x, pltpu.VMEM) for x in results)))


def solution(mesh):
    placed = (
        P("dp", "feat", None),
        P("dp", None),
        P("dp"),
        P("dp"),
        P("dp", "feat"),
        P("dp", "feat"),
        P("dp", "feat"),
        P("feat"),
        P("feat"),
        P("feat"),
    )
    return jax.shard_map(
        body,
        mesh=mesh,
        in_specs=placed,
        out_specs=(P("dp", "feat"), P("dp", "feat"), P("dp", "feat"), P("dp", None)),
        check_vma=False,
    )
```

```python
import functools
import jax
import jax.numpy as jnp
from jax import lax
from jax.experimental import pallas as pl
from jax.experimental.pallas import tpu as pltpu
from jax.sharding import PartitionSpec as P

step_size = 0.1
LANES = 128
PARTS = 2
CHUNKS = 4
MESH = pl.DeviceIdType.MESH
BF16 = jnp.bfloat16
F32 = jnp.float32


def iota(shape, dim):
    return lax.broadcasted_iota(jnp.int32, shape, dim)


def split(x):
    hi = x.astype(BF16)
    return hi, (x - hi.astype(F32)).astype(BF16)


def nt_dot(a, b):
    return lax.dot_general(a, b, (((1,), (1,)), ((), ())), preferred_element_type=F32)


def kernel(
    n, nf, chains, quarter,
    obs_hbm, lab_hbm, live_hbm, grp_hbm, pos_hbm, mom_hbm, grad_hbm, mean_hbm, prec_hbm, mass_hbm,
    newpos_ref, newmom_ref, newgrad_ref, energy_ref,
    lab_in, live_ref, grp_ref, pos_ref, mom_ref, grad_ref, mean_ref, pair_ref,
    lab_ref, par_ref, obs, perm, back, hand, wall, half_ref, state_ref, tot_send, tot_recv, gather_ref, hot_ref, sum_ref, lhs, mine, pair_send, pair_recv,
    far_send, far_recv, res_own, res_recv, nll_ref, dmat, acc, gsend0, gsend1, nsend, grecv0, grecv1, nrecv, esend, erecv,
    in_sem, h_rsem, w_rsem, t_sem, p_rsem, f_rsem, g_rsem, e_rsem, s_rsem,
):
    h_ssem, w_ssem, p_ssem, f_ssem = (in_sem.at[i:j] for i, j in ((0, 1), (1, 3), (3, 4), (4, 5)))
    r_ssem, g_ssem, e_ssem = (in_sem.at[i:j] for i, j in ((5, 6), (6, 9), (9, 10)))
    r_rsem = t_sem.at[0]
    me = lax.axis_index("dp")
    feat = lax.axis_index("feat")
    tiles = lab_ref.shape[0]
    own, width = pos_ref.shape
    pack = LANES // quarter
    part_chains = chains // PARTS
    part_width = width // PARTS
    octet = 2 * pack
    orows = octet * part_chains
    half_octets = tiles // octet // 2
    chunk_octets = half_octets // CHUNKS
    chunk_tiles = chunk_octets * octet
    crows = chunk_octets * orows
    groups = n * own
    bit = feat % 2
    near = feat + 1 - 2 * bit
    far = (feat + nf // 2) % nf

    barrier = pltpu.get_barrier_semaphore()

    def above(body):
        def step(i, carry):
            body(n - 1 - i)
            return carry

        lax.fori_loop(0, n - 1 - me, step, 0)

    def below(body):
        def step(d, carry):
            body(d)
            return carry

        lax.fori_loop(0, me, step, 0)

    def others(body):
        above(body)
        below(body)

    def greet(d):
        pl.semaphore_signal(barrier, inc=1, device_id={"dp": d}, device_id_type=MESH)

    leads = bit == 1
    follows = bit == 0

    @pl.when(leads)
    def _():
        below(greet)

    above(greet)
    for i in range(1, nf):
        pl.semaphore_signal(barrier, inc=1, device_id={"feat": (feat + i) % nf}, device_id_type=MESH)

    sources = [
        (mass_hbm, pair_ref.at[1:2]), (prec_hbm, pair_ref.at[0:1]),
        (mom_hbm, mom_ref), (grad_hbm, grad_ref), (pos_hbm, pos_ref), (mean_hbm, mean_ref),
        (grp_hbm, grp_ref), (live_hbm, live_ref), (lab_hbm, lab_in), (obs_hbm, obs),
    ]
    fetches = [pltpu.make_async_copy(a, b, in_sem.at[i]) for i, (a, b) in enumerate(sources)]
    for f in fetches:
        f.start()

    spread = (iota((quarter, width), 0) == iota((quarter, width), 1) // chains).astype(F32)
    r, c = iota((width, width), 0), iota((width, width), 1)
    perm[...] = jnp.where(
        (r % chains == c // quarter) & (r // chains == c % quarter), 1.0, 0.0
    ).astype(BF16)
    for f in fetches[:5]:
        f.wait()
    par_ref[...] = jnp.dot(
        pair_ref[...], spread, precision=lax.Precision.HIGHEST, preferred_element_type=F32
    )
    half = mom_ref[...] - 0.5 * step_size * grad_ref[...]
    half_ref[...] = half
    moved = pos_ref[...] + step_size * par_ref[1:2, :] * half
    newpos_ref[...] = moved
    coeff = jnp.dot(moved.astype(BF16), perm[...], preferred_element_type=F32).astype(BF16)

    back[...] = jnp.where(
        (c % chains == r // quarter) & (c // chains == r % quarter), 1.0, 0.0
    ).astype(BF16)

    def block(d):
        return pl.ds(pl.multiple_of(d * own, own), own)

    for h in range(PARTS):
        hand[h] = coeff[:, h * part_width:(h + 1) * part_width]

    for h in range(PARTS):
        wall[0, h, block(me), :] = hand[h]
    pl.semaphore_wait(barrier, me + (n - 1 - me) * bit + nf - 1)

    def remote(src, dst, ssem, rsem, to):
        return pltpu.make_async_remote_copy(
            src_ref=src, dst_ref=dst, send_sem=ssem, recv_sem=rsem,
            device_id=to, device_id_type=MESH,
        )

    def hand_copy(h):
        return remote(
            hand.at[h], wall.at[1, h, block(me)], h_ssem.at[0], h_rsem.at[0], {"feat": near}
        )

    def w_copy(h, to, ssem):
        rows = wall.at[0, h, block(me)]
        return remote(rows, rows, ssem, w_rsem.at[h], {"dp": to})

    def t_copy(h, d, to):
        rows = wall.at[1, h, block(d)]
        return remote(rows, rows, w_ssem.at[1], t_sem.at[h, d], {"dp": to})

    def w_all(h):
        blocks = wall.at[0, h, pl.ds(0, (n - 1) * own)]
        return remote(blocks, blocks, w_ssem.at[0], w_rsem.at[h], {"dp": (me + 1) % n})

    def sent(side):
        blocks = wall.at[side, :, pl.ds(0, (n - 1) * own)]
        return remote(blocks, blocks, w_ssem.at[side], w_rsem.at[0], {"dp": (me + 1) % n})

    def pass_on(h, d):
        return remote(
            wall.at[1, h, block(d)], wall.at[0, h, block(d)], w_ssem.at[1], w_rsem.at[h],
            {"feat": near},
        )

    hand_all = remote(hand, hand, h_ssem.at[0], h_rsem.at[0], {"feat": near})

    @pl.when(jnp.logical_not(leads))
    def _():
        for h in range(PARTS):
            hand_copy(h).start()
        for h in range(PARTS):
            below(lambda d: w_copy(h, d, t_sem.at[h, d]).start())

    def send_both(h, d):
        t_copy(h, me, d).start()
        w_copy(h, d, w_ssem.at[0]).start()

    @pl.when(leads)
    def _():
        for h in range(PARTS):
            below(lambda d: w_copy(h, d, w_ssem.at[0]).start())
        hand_all.wait_recv()
        for h in range(PARTS):
            above(lambda d: send_both(h, d))

    square = iota((tiles, tiles), 0) == iota((tiles, tiles), 1)

    def column(row):
        return jnp.sum(jnp.where(square, row.astype(F32), 0.0), axis=1, keepdims=True)

    for f in fetches[5:9]:
        f.wait()
    hot_ref[...] = (
        iota((tiles, groups), 1).astype(F32) == column(grp_ref[...])
    ).astype(F32).astype(BF16)
    member = (iota((groups, tiles), 0) == grp_ref[...]).astype(F32).astype(BF16)
    for i in range(2):
        side = member[:, i * (tiles // 2):(i + 1) * (tiles // 2)]
        sum_ref[i] = jnp.concatenate([side, side], axis=1)
    lab_ref[...] = jnp.where(
        iota(lab_ref.shape, 1).astype(F32) < column(live_ref[...]), lab_in[...].astype(F32), -1.0
    )
    nll_ref[...] = jnp.zeros_like(nll_ref)
    offset = newpos_ref[...] - mean_ref[...]
    force = par_ref[0:1, :] * offset
    drift = half_ref[...] - 0.5 * step_size * force
    high, rest = split(drift)
    low = (drift - high.astype(F32) - rest.astype(F32)).astype(BF16)
    packed = jnp.dot(
        jnp.concatenate([high, rest, low], axis=0), perm[...], preferred_element_type=F32
    )
    state_ref[0, :own, :] = packed[:own] + packed[own:2 * own] + packed[2 * own:]
    lane_mass = jnp.dot(
        pair_ref[...], (iota((quarter, width), 0) == iota((quarter, width), 1) % quarter).astype(F32),
        precision=lax.Precision.HIGHEST, preferred_element_type=F32,
    )[1:2, :]
    state_ref[0, own:own + 8, :] = jnp.broadcast_to(0.5 * lane_mass, (8, width))
    gather_ref[...] = (
        iota((width, LANES), 0) // quarter == iota((width, LANES), 1)
    ).astype(F32).astype(BF16)
    prior = 0.5 * force * offset
    e0 = prior[:, :LANES]
    for m in range(1, width // LANES):
        e0 = e0 + prior[:, m * LANES:(m + 1) * LANES]
    shift = LANES // 2
    while shift >= chains:
        e0 = e0 + pltpu.roll(e0, shift, 1)
        shift //= 2
    state_ref[0, own + 8:, :] = jnp.concatenate([e0] * (width // LANES), axis=1)
    fetches[9].wait()
    state_copy = remote(state_ref.at[0], state_ref.at[1], e_ssem.at[0], s_rsem.at[0], {"feat": near})
    pl.when(follows)(lambda: state_copy.start())

    half_tiles = tiles // 2
    row_t, lane_t = iota((tiles, LANES), 0), iota((tiles, LANES), 1)
    place = row_t % pack
    keep = lane_t // quarter == place
    sides = (keep & (row_t % octet < pack), keep & (row_t % octet >= pack))
    mine_first, near_first = bit * half_tiles, (1 - bit) * half_tiles

    def hand_over(h, d):
        t_copy(h, d, d).wait_recv()
        pass_on(h, d).start()

    def relay(h):
        @pl.when(leads)
        def _():
            below(lambda d: hand_over(h, d))

    def pick(h):
        picked = jnp.dot(hot_ref[...], wall[0, h], preferred_element_type=F32)
        for m in range(part_width // LANES):
            x = picked[:, m * LANES:(m + 1) * LANES]
            turned = [x] + [pltpu.roll(x, s * quarter, 1) for s in range(1, pack)]
            spots = []
            for j in range(pack):
                y = turned[0]
                for s in range(1, pack):
                    y = jnp.where((place + pack - j) % pack == s, turned[s], y)
                spots.append(y)
            for j in range(0, pack, 2):
                at = (m * pack + j) * octet
                for i, side in enumerate(sides):
                    two = jnp.concatenate([
                        jnp.where(side, y, 0.0).reshape(tiles // octet, octet, LANES)
                        for y in spots[j:j + 2]
                    ], axis=1)
                    lhs[h, :, at:at + 2 * octet, i * LANES:(i + 1) * LANES] = two.astype(BF16)

    def logits(h, first_octet, dst, base):
        for i in range(chunk_octets):
            o = first_octet + i
            dst[base + i * orows:base + (i + 1) * orows, :] = jnp.dot(
                lhs[h, o], obs[o], preferred_element_type=F32
            ).astype(dst.dtype)

    units = PARTS * CHUNKS

    def rows(u):
        return pl.ds(u * crows, crows)

    def exchange(src, dst, ssem, rsem, to):
        def copy(u):
            at = pl.ds(u * crows, crows)
            return remote(src.at[at], dst.at[at], ssem.at[0], rsem.at[u], {"feat": to})

        def drain():
            pltpu.make_async_remote_copy(
                src_ref=src, dst_ref=dst, send_sem=ssem.at[0], recv_sem=rsem.at[0],
                device_id={"feat": to}, device_id_type=MESH,
            ).wait_send()

        return copy, drain

    pair_copy, pair_drain = exchange(pair_send, pair_recv, p_ssem, p_rsem, near)
    far_copy, far_drain = exchange(far_send, far_recv, f_ssem, f_rsem, far)
    res_copy, res_drain = exchange(res_own, res_recv, r_ssem, r_rsem, near)

    for h in range(PARTS):
        if h == 0:
            relay(h)

        w_all(h).wait_recv()
        pl.when(jnp.logical_not(leads))(
            lambda: below(lambda d: w_copy(h, d, t_sem.at[h, d]).wait_send())
        )
        pick(h)
        mark = h * CHUNKS
        for k in range(CHUNKS):
            logits(h, (1 - bit) * half_octets + k * chunk_octets, pair_send, (mark + k) * crows)
        for u in range(mark, mark + CHUNKS):
            pair_copy(u).start()
        if h + 1 < PARTS:
            relay(h + 1)
        for k in range(CHUNKS):
            logits(h, bit * half_octets + k * chunk_octets, mine, (mark + k) * crows)
        for u in range(mark, mark + CHUNKS):
            pair_copy(u).wait_recv()
            total = mine[rows(u), :] + pair_recv[rows(u), :].astype(F32)
            mine[rows(u), :] = total
            far_send[rows(u), :] = total.astype(BF16)
            far_copy(u).start()

    spot = iota((orows, LANES), 0) % octet
    diag = tuple(spot == iota((orows, LANES), 1) // quarter + i * pack for i in range(2))

    def grads(h, first_octet, src, base):
        for i in range(chunk_octets):
            o = first_octet + i
            g = nt_dot(src[base + i * orows:base + (i + 1) * orows, :], obs[o])
            g = jnp.where(diag[0], g[:, :LANES], jnp.where(diag[1], g[:, LANES:], 0.0))
            tile = pl.ds(pl.multiple_of(o * octet, octet), octet)
            dmat[h * part_chains:(h + 1) * part_chains, tile, :] = g.reshape(part_chains, octet, LANES)

    def residual(u):
        h, k = divmod(u, CHUNKS)
        z = mine[rows(u), :] + far_recv[rows(u), :].astype(F32)
        first = pl.multiple_of((bit * half_octets + k * chunk_octets) * octet, chunk_tiles)
        lab = lab_ref[pl.ds(first, chunk_tiles), :]
        lab = lab.reshape(chunk_octets, 1, octet, LANES)
        lab = jnp.broadcast_to(lab, (chunk_octets, part_chains, octet, LANES)).reshape(crows, LANES)
        live = lab >= 0.0
        e = jnp.exp(-jnp.abs(z))
        inv = 1.0 / (1.0 + e)
        sig = jnp.where(z >= 0.0, inv, e * inv)
        res_own[rows(u), :] = jnp.where(live, sig - lab, 0.0).astype(BF16)
        res_copy(u).start()
        v = jnp.where(live, jnp.maximum(z, 0.0) + jnp.log(1.0 + e) - lab * z, 0.0)
        s = jnp.sum(v, axis=1, keepdims=True) * (2.0 / nf)
        at = iota((crows, LANES), 0) // octet % part_chains + h * part_chains == iota((crows, LANES), 1)
        s = jnp.where(at, s, 0.0).reshape(chunk_octets, part_chains, octet, LANES)
        nll_ref[pl.ds(first, chunk_tiles), :] += jnp.sum(s, axis=1).reshape(chunk_tiles, LANES)

    def mine_grads(u):
        h, k = divmod(u, CHUNKS)
        grads(h, bit * half_octets + k * chunk_octets, res_own, u * crows)

    def near_grads(u):
        h, k = divmod(u, CHUNKS)
        grads(h, (1 - bit) * half_octets + k * chunk_octets, res_recv, u * crows)

    seg_groups = min(groups, LANES)
    lane_g = iota((half_tiles, LANES), 1) // quarter
    blocks = part_width // LANES
    sums = ((gsend0, grecv0), (gsend1, grecv1), (nsend, nrecv))

    def stacked(d):
        return jnp.concatenate(split(d), axis=0)

    def fold(xs, width):
        if len(xs) == 1:
            return xs[0]
        half = len(xs) // 2
        shift = half * width
        low = lane_g % len(xs) < half
        pairs = []
        for a, b in zip(xs[:half], xs[half:]):
            other = jnp.where(low, b, a)
            if len(xs) == pack:
                moved = pltpu.roll(other, shift, 1)
            else:
                moved = jnp.where(
                    low, pltpu.roll(other, LANES - shift, 1), pltpu.roll(other, shift, 1)
                )
            pairs.append(jnp.where(low, a, b) + moved)
        return fold(pairs, width)

    def compact(h, first):
        out = []
        for m in range(blocks):
            xs = []
            for j in range(pack):
                tile = pl.ds(pl.multiple_of(first, half_tiles), half_tiles)
                xs.append(dmat[h * part_chains + m * pack + j, tile, :])
            out.append(fold(xs, quarter))
        return stacked(jnp.concatenate(out, axis=1))

    def over_groups(body):
        def run(gc, carry):
            body(pl.ds(pl.multiple_of(gc * seg_groups, seg_groups), seg_groups))
            return carry

        if groups == seg_groups:
            body(pl.ds(0, groups))
        else:
            lax.fori_loop(0, groups // seg_groups, run, 0)

    def member_dot(side, out, rhs):
        return jnp.dot(sum_ref[side, out, :], rhs, preferred_element_type=F32)

    def start_half(h):
        rhs = compact(h, mine_first)
        nll = None
        if h == PARTS - 1:
            nll = stacked(nll_ref[pl.ds(pl.multiple_of(mine_first, half_tiles), half_tiles), :])

        def body(out):
            acc[out, :] = member_dot(bit, out, rhs)
            if nll is not None:
                hi, lo = split(member_dot(bit, out, nll))
                nsend[out, :] = (
                    hi.astype(F32) + pltpu.roll(lo.astype(F32), chains, 1)
                ).astype(BF16)

        over_groups(body)

    def whole(h):
        rhs = compact(h, mine_first), compact(h, near_first)

        def body(out):
            sums[h][0][out, :] = (
                member_dot(bit, out, rhs[0]) + member_dot(1 - bit, out, rhs[1])
            ).astype(BF16)

        over_groups(body)

    def finish_half(h):
        rhs = compact(h, near_first)

        def body(out):
            sums[h][0][out, :] = (acc[out, :] + member_dot(1 - bit, out, rhs)).astype(BF16)

        over_groups(body)

    def g_copy(h, to):
        return remote(
            sums[h][0].at[block(to)], sums[h][1].at[1 - bit, me], g_ssem.at[h], g_rsem.at[1 - bit, h],
            {"dp": to, "feat": feat + 1 - bit},
        )

    def g_all(h, side, count):
        got = sums[h][1].at[side, pl.ds(0, count)]
        return remote(got, got, g_ssem.at[h], g_rsem.at[side, h], {"feat": near})

    def send_sums(h):
        others(lambda d: g_copy(h, d).start())

        @pl.when(leads)
        def _():
            sums[h][1][0, me] = sums[h][0][block(me), :]

        pl.when(follows)(lambda: g_copy(h, me).start())

    lag = 2
    for u in range(units):
        far_copy(u).wait_recv()
        if u >= lag:
            res_copy(u - lag).wait_recv()
        residual(u)
        mine_grads(u)
        if u >= lag:
            near_grads(u - lag)
            h, k = divmod(u - lag, CHUNKS)
            if k == CHUNKS - 1:
                whole(h)
                send_sums(h)
    for u in range(units - lag, units - 1):
        res_copy(u).wait_recv()
        near_grads(u)
    start_half(PARTS - 1)
    send_sums(PARTS)
    res_copy(units - 1).wait_recv()
    near_grads(units - 1)
    finish_half(PARTS - 1)
    send_sums(PARTS - 1)

    def total_of(h, side):
        g_all(h, side, n - 1 + side).wait_recv()
        return jnp.sum(sums[h][1][side].astype(F32), axis=0)

    def natural(packed, h):
        parts = jnp.concatenate(split(packed), axis=0)
        both = jnp.dot(
            parts, back[h * part_width:(h + 1) * part_width, :], preferred_element_type=F32
        )
        return both[:own] + both[own:]

    def write(totals):
        new_gradient = par_ref[0:1, :] * (newpos_ref[...] - mean_ref[...])
        for h in range(PARTS):
            new_gradient = new_gradient + natural(totals[h], h)
        newgrad_ref[...] = new_gradient
        newmom_ref[...] = half_ref[...] - 0.5 * step_size * new_gradient

    tot_copy = remote(tot_send, tot_recv, h_ssem.at[0], s_rsem.at[0], {"feat": near})

    def e_copy(i):
        return remote(
            esend, erecv.at[feat // 2], e_ssem.at[0], e_rsem.at[0], {"feat": (feat + i) % nf}
        )

    def e_all(count):
        got = erecv.at[pl.ds(0, count)]
        return remote(got, got, e_ssem.at[0], e_rsem.at[0], {"feat": near})

    def drain_all(count):
        for drain in (pair_drain, far_drain, res_drain):
            drain()
        for h in range(PARTS + 1):
            g_all(h, 0, count).wait_send()

    @pl.when(leads)
    def _():
        state_copy.wait_recv()
        energy = state_ref[0, own + 8:, :LANES] + state_ref[1, own + 8:, :LANES]
        totals = []
        for h in range(PARTS):
            if h == PARTS - 1:
                loss = total_of(PARTS, 0) + total_of(PARTS, 1)
                energy = energy + loss + pltpu.roll(loss, LANES - chains, 1)
            cols = slice(h * part_width, (h + 1) * part_width)
            squares = []
            for side in range(2):
                total = total_of(h, side)
                if side:
                    tot_send[h] = total
                else:
                    totals.append(total)
                t = state_ref[side, :own, cols] - 0.5 * step_size * total
                squares.append(state_ref[side, own:own + 1, cols] * t * t)
            both = jnp.dot(
                stacked(squares[0] + squares[1]), gather_ref[cols, :], preferred_element_type=F32
            )
            energy = energy + both[:own] + both[own:]
        esend[...] = energy
        for i in range(1, nf):
            e_copy(i).start()
        tot_copy.start()
        erecv[feat // 2] = esend[...]
        write(totals)
        drain_all(n - 1)
        for side in range(2):
            sent(side).wait_send()
        tot_copy.wait_send()
        sent_e = state_ref.at[1, pl.ds(0, 8 * (nf - 1)), pl.ds(0, own * LANES // 8)]
        remote(sent_e, sent_e, e_ssem.at[0], e_rsem.at[0], {"feat": near}).wait_send()
        if nf > 2:
            e_all(nf // 2 - 1).wait_recv()

    @pl.when(follows)
    def _():
        tot_copy.wait_recv()
        write([tot_recv[h] for h in range(PARTS)])
        drain_all(n)
        hand_all.wait_send()
        state_copy.wait_send()
        e_all(nf // 2).wait_recv()

    e = erecv[0]
    for i in range(1, nf // 2):
        e = e + erecv[i]
    energy_ref[...] = e[:, :chains]


def finish(*refs):
    sem = refs[8]
    copies = [pltpu.make_async_copy(refs[i], refs[4 + i], sem.at[i]) for i in range(4)]
    for c in copies:
        c.start()
    for c in copies:
        c.wait()


def body(observations, labels, tile_live, tile_group, position, momentum, gradient, prior_mean, prior_prec, inv_mass):
    n, nf = lax.axis_size("dp"), lax.axis_size("feat")
    tiles, quarter, row_count = observations.shape
    own, width = position.shape
    chains = width // quarter
    pack = LANES // quarter
    half_rows = tiles * chains // 2
    anywhere = pl.BlockSpec(memory_space=pl.ANY)
    units = PARTS * CHUNKS
    dma = pltpu.SemaphoreType.DMA
    block = pltpu.VMEM((own, width), F32)
    results = pl.pallas_call(
        functools.partial(kernel, n, nf, chains, quarter),
        out_shape=(block, block, block, pltpu.VMEM((own, chains), F32)),
        in_specs=[anywhere] * 10,
        out_specs=(pl.BlockSpec(memory_space=pltpu.VMEM),) * 4,
        scratch_shapes=[
            pltpu.VMEM((tiles, row_count), jnp.int32),
            pltpu.VMEM((1, tiles), jnp.int32),
            pltpu.VMEM((1, tiles), jnp.int32),
            pltpu.VMEM((own, width), F32),
            pltpu.VMEM((own, width), F32),
            pltpu.VMEM((own, width), F32),
            pltpu.VMEM((1, width), F32),
            pltpu.VMEM((2, quarter), F32),
            pltpu.VMEM((tiles, row_count), F32),
            pltpu.VMEM((2, width), F32),
            pltpu.VMEM((tiles // pack // 2, 2 * LANES, row_count), BF16),
            pltpu.VMEM((width, width), BF16),
            pltpu.VMEM((width, width), BF16),
            pltpu.VMEM((PARTS, own, width // PARTS), BF16),
            pltpu.VMEM((2, PARTS, n * own, width // PARTS), BF16),
            pltpu.VMEM((own, width), F32),
            pltpu.VMEM((2, 2 * own + 8, width), F32),
            pltpu.VMEM((PARTS, own, width // PARTS), F32),
            pltpu.VMEM((PARTS, own, width // PARTS), F32),
            pltpu.VMEM((width, LANES), BF16),
            pltpu.VMEM((tiles, n * own), BF16),
            pltpu.VMEM((2, n * own, tiles), BF16),
            pltpu.VMEM((PARTS, tiles // pack // 2, 2 * pack * chains // PARTS, 2 * LANES), BF16),
            pltpu.VMEM((half_rows, row_count), F32),
            pltpu.VMEM((half_rows, row_count), F32),
            pltpu.VMEM((half_rows, row_count), F32),
            pltpu.VMEM((half_rows, row_count), BF16),
            pltpu.VMEM((half_rows, row_count), BF16),
            pltpu.VMEM((half_rows, row_count), BF16),
            pltpu.VMEM((half_rows, row_count), BF16),
            pltpu.VMEM((tiles, LANES), F32),
            pltpu.VMEM((chains, tiles, LANES), F32),
            pltpu.VMEM((n * own, width // PARTS), F32),
            pltpu.VMEM((n * own, width // PARTS), BF16),
            pltpu.VMEM((n * own, width // PARTS), BF16),
            pltpu.VMEM((n * own, LANES), BF16),
            pltpu.VMEM((2, n, own, width // PARTS), BF16),
            pltpu.VMEM((2, n, own, width // PARTS), BF16),
            pltpu.VMEM((2, n, own, LANES), BF16),
            pltpu.VMEM((own, LANES), F32),
            pltpu.VMEM((nf // 2, own, LANES), F32),
            dma((10,)),
            dma((1,)), dma((PARTS,)), dma((PARTS, max(n, units))),
            dma((units,)), dma((units,)), dma((2, PARTS + 1)), dma((1,)), dma((1,)),
        ],
        compiler_params=pltpu.CompilerParams(collective_id=0, has_side_effects=True),
    )(
        observations.reshape(tiles // pack // 2, 2 * LANES, row_count),
        labels, tile_live.reshape(1, tiles), tile_group.reshape(1, tiles),
        position, momentum, gradient,
        prior_mean.reshape(1, width), prior_prec.reshape(1, quarter), inv_mass.reshape(1, quarter),
    )
    return tuple(pl.pallas_call(
        finish,
        out_shape=tuple(jax.ShapeDtypeStruct(x.shape, x.dtype) for x in results),
        in_specs=[pl.BlockSpec(memory_space=pltpu.VMEM)] * 4,
        out_specs=(anywhere,) * 4,
        scratch_shapes=[dma((4,))],
    )(*(pltpu.with_memory_space_constraint(x, pltpu.VMEM) for x in results)))


def solution(mesh):
    placed = (
        P("dp", "feat", None),
        P("dp", None),
        P("dp"),
        P("dp"),
        P("dp", "feat"),
        P("dp", "feat"),
        P("dp", "feat"),
        P("feat"),
        P("feat"),
        P("feat"),
    )
    return jax.shard_map(
        body,
        mesh=mesh,
        in_specs=placed,
        out_specs=(P("dp", "feat"), P("dp", "feat"), P("dp", "feat"), P("dp", None)),
        check_vma=False,
    )
```

```python
import functools
import jax
import jax.numpy as jnp
from jax import lax
from jax.experimental import pallas as pl
from jax.experimental.pallas import tpu as pltpu
from jax.sharding import PartitionSpec as P

step_size = 0.1
LANES = 128
PARTS = 2
CHUNKS = 4
MESH = pl.DeviceIdType.MESH
BF16 = jnp.bfloat16
F32 = jnp.float32


def iota(shape, dim):
    return lax.broadcasted_iota(jnp.int32, shape, dim)


def split(x):
    hi = x.astype(BF16)
    return hi, (x - hi.astype(F32)).astype(BF16)


def nt_dot(a, b):
    return lax.dot_general(a, b, (((1,), (1,)), ((), ())), preferred_element_type=F32)


def kernel(
    n, nf, chains, quarter,
    obs_hbm, lab_hbm, live_hbm, grp_hbm, pos_hbm, mom_hbm, grad_hbm, mean_hbm, prec_hbm, mass_hbm,
    newpos_ref, newmom_ref, newgrad_ref, energy_ref,
    lab_in, live_ref, grp_ref, pos_ref, mom_ref, grad_ref, mean_ref, pair_ref,
    lab_ref, par_ref, obs, perm, back, hand, wall, half_ref, state_ref, tot_send, tot_recv, gather_ref, hot_ref, sum_ref, most_ref, last_ref, lhs, mine, pair_send, pair_recv,
    far_send, far_recv, res_own, res_recv, nll_ref, dmat, acc, gsend0, gsend1, nsend, grecv0, grecv1, nrecv, esend, erecv,
    in_sem, h_rsem, w_rsem, t_sem, p_rsem, f_rsem, g_rsem, e_rsem, s_rsem,
):
    h_ssem, w_ssem, p_ssem, f_ssem = (in_sem.at[i:j] for i, j in ((0, 1), (1, 3), (3, 4), (4, 5)))
    r_ssem, g_ssem, e_ssem = (in_sem.at[i:j] for i, j in ((5, 6), (6, 9), (9, 10)))
    r_rsem = t_sem.at[0]
    me = lax.axis_index("dp")
    feat = lax.axis_index("feat")
    tiles = lab_ref.shape[0]
    own, width = pos_ref.shape
    pack = LANES // quarter
    part_chains = chains // PARTS
    part_width = width // PARTS
    octet = 2 * pack
    orows = octet * part_chains
    half_octets = tiles // octet // 2
    chunk_octets = half_octets // CHUNKS
    chunk_tiles = chunk_octets * octet
    crows = chunk_octets * orows
    groups = n * own
    bit = feat % 2
    near = feat + 1 - 2 * bit
    far = (feat + nf // 2) % nf

    barrier = pltpu.get_barrier_semaphore()

    def above(body):
        def step(i, carry):
            body(n - 1 - i)
            return carry

        lax.fori_loop(0, n - 1 - me, step, 0)

    def below(body):
        def step(d, carry):
            body(d)
            return carry

        lax.fori_loop(0, me, step, 0)

    def others(body):
        above(body)
        below(body)

    def greet(d):
        pl.semaphore_signal(barrier, inc=1, device_id={"dp": d}, device_id_type=MESH)

    leads = bit == 1
    follows = bit == 0

    @pl.when(leads)
    def _():
        below(greet)

    above(greet)
    for i in range(1, nf):
        pl.semaphore_signal(barrier, inc=1, device_id={"feat": (feat + i) % nf}, device_id_type=MESH)

    sources = [
        (mass_hbm, pair_ref.at[1:2]), (prec_hbm, pair_ref.at[0:1]),
        (mom_hbm, mom_ref), (grad_hbm, grad_ref), (pos_hbm, pos_ref), (mean_hbm, mean_ref),
        (grp_hbm, grp_ref), (live_hbm, live_ref), (lab_hbm, lab_in), (obs_hbm, obs),
    ]
    fetches = [pltpu.make_async_copy(a, b, in_sem.at[i]) for i, (a, b) in enumerate(sources)]
    for f in fetches:
        f.start()

    spread = (iota((quarter, width), 0) == iota((quarter, width), 1) // chains).astype(F32)
    r, c = iota((width, width), 0), iota((width, width), 1)
    perm[...] = jnp.where(
        (r % chains == c // quarter) & (r // chains == c % quarter), 1.0, 0.0
    ).astype(BF16)
    for f in fetches[:5]:
        f.wait()
    par_ref[...] = jnp.dot(
        pair_ref[...], spread, precision=lax.Precision.HIGHEST, preferred_element_type=F32
    )
    half = mom_ref[...] - 0.5 * step_size * grad_ref[...]
    half_ref[...] = half
    moved = pos_ref[...] + step_size * par_ref[1:2, :] * half
    newpos_ref[...] = moved
    coeff = jnp.dot(moved.astype(BF16), perm[...], preferred_element_type=F32).astype(BF16)

    back[...] = jnp.where(
        (c % chains == r // quarter) & (c // chains == r % quarter), 1.0, 0.0
    ).astype(BF16)

    def block(d):
        return pl.ds(pl.multiple_of(d * own, own), own)

    for h in range(PARTS):
        hand[h] = coeff[:, h * part_width:(h + 1) * part_width]

    for h in range(PARTS):
        wall[0, h, block(me), :] = hand[h]
    pl.semaphore_wait(barrier, me + (n - 1 - me) * bit + nf - 1)

    def remote(src, dst, ssem, rsem, to):
        return pltpu.make_async_remote_copy(
            src_ref=src, dst_ref=dst, send_sem=ssem, recv_sem=rsem,
            device_id=to, device_id_type=MESH,
        )

    def hand_copy(h):
        return remote(
            hand.at[h], wall.at[1, h, block(me)], h_ssem.at[0], h_rsem.at[0], {"feat": near}
        )

    def w_copy(h, to, ssem):
        rows = wall.at[0, h, block(me)]
        return remote(rows, rows, ssem, w_rsem.at[h], {"dp": to})

    def t_copy(h, d, to):
        rows = wall.at[1, h, block(d)]
        return remote(rows, rows, w_ssem.at[1], t_sem.at[h, d], {"dp": to})

    def w_all(h):
        blocks = wall.at[0, h, pl.ds(0, (n - 1) * own)]
        return remote(blocks, blocks, w_ssem.at[0], w_rsem.at[h], {"dp": (me + 1) % n})

    def sent(side):
        blocks = wall.at[side, :, pl.ds(0, (n - 1) * own)]
        return remote(blocks, blocks, w_ssem.at[side], w_rsem.at[0], {"dp": (me + 1) % n})

    def pass_on(h, d):
        return remote(
            wall.at[1, h, block(d)], wall.at[0, h, block(d)], w_ssem.at[1], w_rsem.at[h],
            {"feat": near},
        )

    hand_all = remote(hand, hand, h_ssem.at[0], h_rsem.at[0], {"feat": near})

    @pl.when(jnp.logical_not(leads))
    def _():
        for h in range(PARTS):
            hand_copy(h).start()
        for h in range(PARTS):
            below(lambda d: w_copy(h, d, t_sem.at[h, d]).start())

    def send_both(h, d):
        t_copy(h, me, d).start()
        w_copy(h, d, w_ssem.at[0]).start()

    @pl.when(leads)
    def _():
        for h in range(PARTS):
            below(lambda d: w_copy(h, d, w_ssem.at[0]).start())
        hand_all.wait_recv()
        for h in range(PARTS):
            above(lambda d: send_both(h, d))

    square = iota((tiles, tiles), 0) == iota((tiles, tiles), 1)

    def column(row):
        return jnp.sum(jnp.where(square, row.astype(F32), 0.0), axis=1, keepdims=True)

    for f in fetches[5:9]:
        f.wait()
    hot_ref[...] = (
        iota((tiles, groups), 1).astype(F32) == column(grp_ref[...])
    ).astype(F32).astype(BF16)
    member = (iota((groups, tiles), 0) == grp_ref[...]).astype(F32).astype(BF16)
    for i in range(2):
        side = member[:, i * (tiles // 2):(i + 1) * (tiles // 2)]
        sum_ref[i] = jnp.concatenate([side, side], axis=1)
        most_ref[i] = jnp.concatenate([side[:, :-chunk_tiles]] * 2, axis=1)
        last_ref[i] = jnp.concatenate([side[:, -chunk_tiles:]] * 2, axis=1)
    lab_ref[...] = jnp.where(
        iota(lab_ref.shape, 1).astype(F32) < column(live_ref[...]), lab_in[...].astype(F32), -1.0
    )
    nll_ref[...] = jnp.zeros_like(nll_ref)
    offset = newpos_ref[...] - mean_ref[...]
    force = par_ref[0:1, :] * offset
    drift = half_ref[...] - 0.5 * step_size * force
    high, rest = split(drift)
    low = (drift - high.astype(F32) - rest.astype(F32)).astype(BF16)
    packed = jnp.dot(
        jnp.concatenate([high, rest, low], axis=0), perm[...], preferred_element_type=F32
    )
    state_ref[0, :own, :] = packed[:own] + packed[own:2 * own] + packed[2 * own:]
    lane_mass = jnp.dot(
        pair_ref[...], (iota((quarter, width), 0) == iota((quarter, width), 1) % quarter).astype(F32),
        precision=lax.Precision.HIGHEST, preferred_element_type=F32,
    )[1:2, :]
    state_ref[0, own:own + 8, :] = jnp.broadcast_to(0.5 * lane_mass, (8, width))
    gather_ref[...] = (
        iota((width, LANES), 0) // quarter == iota((width, LANES), 1)
    ).astype(F32).astype(BF16)
    prior = 0.5 * force * offset
    e0 = prior[:, :LANES]
    for m in range(1, width // LANES):
        e0 = e0 + prior[:, m * LANES:(m + 1) * LANES]
    shift = LANES // 2
    while shift >= chains:
        e0 = e0 + pltpu.roll(e0, shift, 1)
        shift //= 2
    state_ref[0, own + 8:, :] = jnp.concatenate([e0] * (width // LANES), axis=1)
    fetches[9].wait()
    state_copy = remote(state_ref.at[0], state_ref.at[1], e_ssem.at[0], s_rsem.at[0], {"feat": near})
    pl.when(follows)(lambda: state_copy.start())

    half_tiles = tiles // 2
    row_t, lane_t = iota((tiles, LANES), 0), iota((tiles, LANES), 1)
    place = row_t % pack
    keep = lane_t // quarter == place
    sides = (keep & (row_t % octet < pack), keep & (row_t % octet >= pack))
    mine_first, near_first = bit * half_tiles, (1 - bit) * half_tiles

    def hand_over(h, d):
        t_copy(h, d, d).wait_recv()
        pass_on(h, d).start()

    def relay(h):
        @pl.when(leads)
        def _():
            below(lambda d: hand_over(h, d))

    def pick(h):
        picked = jnp.dot(hot_ref[...], wall[0, h], preferred_element_type=F32)
        for m in range(part_width // LANES):
            x = picked[:, m * LANES:(m + 1) * LANES]
            turned = [x] + [pltpu.roll(x, s * quarter, 1) for s in range(1, pack)]
            spots = []
            for j in range(pack):
                y = turned[0]
                for s in range(1, pack):
                    y = jnp.where((place + pack - j) % pack == s, turned[s], y)
                spots.append(y)
            for j in range(0, pack, 2):
                at = (m * pack + j) * octet
                for i, side in enumerate(sides):
                    two = jnp.concatenate([
                        jnp.where(side, y, 0.0).reshape(tiles // octet, octet, LANES)
                        for y in spots[j:j + 2]
                    ], axis=1)
                    lhs[h, :, at:at + 2 * octet, i * LANES:(i + 1) * LANES] = two.astype(BF16)

    def logits(h, first_octet, dst, base):
        for i in range(chunk_octets):
            o = first_octet + i
            dst[base + i * orows:base + (i + 1) * orows, :] = jnp.dot(
                lhs[h, o], obs[o], preferred_element_type=F32
            ).astype(dst.dtype)

    units = PARTS * CHUNKS

    def rows(u):
        return pl.ds(u * crows, crows)

    def exchange(src, dst, ssem, rsem, to):
        def copy(u):
            at = pl.ds(u * crows, crows)
            return remote(src.at[at], dst.at[at], ssem.at[0], rsem.at[u], {"feat": to})

        def drain():
            pltpu.make_async_remote_copy(
                src_ref=src, dst_ref=dst, send_sem=ssem.at[0], recv_sem=rsem.at[0],
                device_id={"feat": to}, device_id_type=MESH,
            ).wait_send()

        return copy, drain

    pair_copy, pair_drain = exchange(pair_send, pair_recv, p_ssem, p_rsem, near)
    far_copy, far_drain = exchange(far_send, far_recv, f_ssem, f_rsem, far)
    res_copy, res_drain = exchange(res_own, res_recv, r_ssem, r_rsem, near)

    for h in range(PARTS):
        if h == 0:
            relay(h)

        w_all(h).wait_recv()
        pl.when(jnp.logical_not(leads))(
            lambda: below(lambda d: w_copy(h, d, t_sem.at[h, d]).wait_send())
        )
        pick(h)
        mark = h * CHUNKS
        for k in range(CHUNKS):
            logits(h, (1 - bit) * half_octets + k * chunk_octets, pair_send, (mark + k) * crows)
        for u in range(mark, mark + CHUNKS):
            pair_copy(u).start()
        if h + 1 < PARTS:
            relay(h + 1)
        for k in range(CHUNKS):
            logits(h, bit * half_octets + k * chunk_octets, mine, (mark + k) * crows)
        for u in range(mark, mark + CHUNKS):
            pair_copy(u).wait_recv()
            total = mine[rows(u), :] + pair_recv[rows(u), :].astype(F32)
            mine[rows(u), :] = total
            far_send[rows(u), :] = total.astype(BF16)
            far_copy(u).start()

    spot = iota((orows, LANES), 0) % octet
    diag = tuple(spot == iota((orows, LANES), 1) // quarter + i * pack for i in range(2))

    def grads(h, first_octet, src, base):
        for i in range(chunk_octets):
            o = first_octet + i
            g = nt_dot(src[base + i * orows:base + (i + 1) * orows, :], obs[o])
            g = jnp.where(diag[0], g[:, :LANES], jnp.where(diag[1], g[:, LANES:], 0.0))
            tile = pl.ds(pl.multiple_of(o * octet, octet), octet)
            dmat[h * part_chains:(h + 1) * part_chains, tile, :] = g.reshape(part_chains, octet, LANES)

    def residual(u):
        h, k = divmod(u, CHUNKS)
        z = mine[rows(u), :] + far_recv[rows(u), :].astype(F32)
        first = pl.multiple_of((bit * half_octets + k * chunk_octets) * octet, chunk_tiles)
        lab = lab_ref[pl.ds(first, chunk_tiles), :]
        lab = lab.reshape(chunk_octets, 1, octet, LANES)
        lab = jnp.broadcast_to(lab, (chunk_octets, part_chains, octet, LANES)).reshape(crows, LANES)
        live = lab >= 0.0
        e = jnp.exp(-jnp.abs(z))
        inv = 1.0 / (1.0 + e)
        sig = jnp.where(z >= 0.0, inv, e * inv)
        res_own[rows(u), :] = jnp.where(live, sig - lab, 0.0).astype(BF16)
        res_copy(u).start()
        v = jnp.where(live, jnp.maximum(z, 0.0) + jnp.log(1.0 + e) - lab * z, 0.0)
        s = jnp.sum(v, axis=1, keepdims=True) * (2.0 / nf)
        at = iota((crows, LANES), 0) // octet % part_chains + h * part_chains == iota((crows, LANES), 1)
        s = jnp.where(at, s, 0.0).reshape(chunk_octets, part_chains, octet, LANES)
        nll_ref[pl.ds(first, chunk_tiles), :] += jnp.sum(s, axis=1).reshape(chunk_tiles, LANES)

    def mine_grads(u):
        h, k = divmod(u, CHUNKS)
        grads(h, bit * half_octets + k * chunk_octets, res_own, u * crows)

    def near_grads(u):
        h, k = divmod(u, CHUNKS)
        grads(h, (1 - bit) * half_octets + k * chunk_octets, res_recv, u * crows)

    seg_groups = min(groups, LANES)
    lane_g = iota((half_tiles, LANES), 1) // quarter
    blocks = part_width // LANES
    sums = ((gsend0, grecv0), (gsend1, grecv1), (nsend, nrecv))

    def stacked(d):
        return jnp.concatenate(split(d), axis=0)

    def fold(xs, width):
        if len(xs) == 1:
            return xs[0]
        half = len(xs) // 2
        shift = half * width
        low = lane_g[:xs[0].shape[0]] % len(xs) < half
        pairs = []
        for a, b in zip(xs[:half], xs[half:]):
            other = jnp.where(low, b, a)
            if len(xs) == pack:
                moved = pltpu.roll(other, shift, 1)
            else:
                moved = jnp.where(
                    low, pltpu.roll(other, LANES - shift, 1), pltpu.roll(other, shift, 1)
                )
            pairs.append(jnp.where(low, a, b) + moved)
        return fold(pairs, width)

    def compact(h, first, start=0, count=None):
        count = count or half_tiles
        out = []
        for m in range(blocks):
            xs = []
            for j in range(pack):
                tile = pl.ds(pl.multiple_of(first + start, octet), count)
                xs.append(dmat[h * part_chains + m * pack + j, tile, :])
            out.append(fold(xs, quarter))
        return stacked(jnp.concatenate(out, axis=1))

    def over_groups(body):
        def run(gc, carry):
            body(pl.ds(pl.multiple_of(gc * seg_groups, seg_groups), seg_groups))
            return carry

        if groups == seg_groups:
            body(pl.ds(0, groups))
        else:
            lax.fori_loop(0, groups // seg_groups, run, 0)

    def member_dot(side, out, rhs):
        return jnp.dot(sum_ref[side, out, :], rhs, preferred_element_type=F32)

    most = half_tiles - chunk_tiles

    def start_half(h):
        rhs = compact(h, mine_first)
        rest = compact(h, near_first, 0, most)
        nll = None
        if h == PARTS - 1:
            nll = stacked(nll_ref[pl.ds(pl.multiple_of(mine_first, half_tiles), half_tiles), :])

        def body(out):
            acc[out, :] = member_dot(bit, out, rhs) + jnp.dot(
                most_ref[1 - bit, out, :], rest, preferred_element_type=F32
            )
            if nll is not None:
                hi, lo = split(member_dot(bit, out, nll))
                loss = hi.astype(F32) + pltpu.roll(lo.astype(F32), chains, 1)
                loss = loss.reshape(seg_groups // own, 2, own // 2, LANES)
                loss = loss[:, 0].reshape(-1, LANES) + pltpu.roll(
                    loss[:, 1].reshape(-1, LANES), 2 * chains, 1
                )
                owners = pl.ds(out.start // own, seg_groups // own)
                nsend[owners] = loss.reshape(-1, own // 2, LANES).astype(BF16)

        over_groups(body)

    def whole(h):
        rhs = compact(h, mine_first), compact(h, near_first)

        def body(out):
            sums[h][0][out, :] = (
                member_dot(bit, out, rhs[0]) + member_dot(1 - bit, out, rhs[1])
            ).astype(BF16)

        over_groups(body)

    def finish_half(h):
        rhs = compact(h, near_first, most, chunk_tiles)

        def body(out):
            sums[h][0][out, :] = (acc[out, :] + jnp.dot(last_ref[1 - bit, out, :], rhs, preferred_element_type=F32)).astype(BF16)

        over_groups(body)

    def g_copy(h, to):
        src = nsend.at[to] if h == PARTS else sums[h][0].at[block(to)]
        return remote(
            src, sums[h][1].at[1 - bit, me], g_ssem.at[h], g_rsem.at[1 - bit, h],
            {"dp": to, "feat": feat + 1 - bit},
        )

    def g_all(h, side, count):
        got = sums[h][1].at[side, pl.ds(0, count)]
        return remote(got, got, g_ssem.at[h], g_rsem.at[side, h], {"feat": near})

    def send_sums(h):
        below(lambda d: g_copy(h, d).start())
        above(lambda d: g_copy(h, d).start())

        @pl.when(leads)
        def _():
            sums[h][1][0, me] = nsend[me] if h == PARTS else sums[h][0][block(me), :]

        pl.when(follows)(lambda: g_copy(h, me).start())

    lag = 2

    def near_step(u):
        res_copy(u).wait_recv()
        near_grads(u)

    for u in range(units):
        if u == units - 1:
            near_step(u - lag)
        far_copy(u).wait_recv()
        if lag <= u < units - 1:
            res_copy(u - lag).wait_recv()
        residual(u)
        mine_grads(u)
        if lag <= u < units - 1:
            near_grads(u - lag)
            h, k = divmod(u - lag, CHUNKS)
            if k == CHUNKS - 1:
                whole(h)
                send_sums(h)
    near_step(units - 2)
    start_half(PARTS - 1)
    send_sums(PARTS)
    near_step(units - 1)
    finish_half(PARTS - 1)
    send_sums(PARTS - 1)

    def total_of(h, side):
        g_all(h, side, n - 1 + side).wait_recv()
        return jnp.sum(sums[h][1][side].astype(F32), axis=0)

    def natural(packed, h):
        parts = jnp.concatenate(split(packed), axis=0)
        both = jnp.dot(
            parts, back[h * part_width:(h + 1) * part_width, :], preferred_element_type=F32
        )
        return both[:own] + both[own:]

    def write(totals):
        new_gradient = par_ref[0:1, :] * (newpos_ref[...] - mean_ref[...])
        for h in range(PARTS):
            new_gradient = new_gradient + natural(totals[h], h)
        newgrad_ref[...] = new_gradient
        newmom_ref[...] = half_ref[...] - 0.5 * step_size * new_gradient

    tot_copy = remote(tot_send, tot_recv, h_ssem.at[0], s_rsem.at[0], {"feat": near})

    def e_copy(i):
        return remote(
            esend, erecv.at[feat // 2], e_ssem.at[0], e_rsem.at[0], {"feat": (feat + i) % nf}
        )

    def e_all(count):
        got = erecv.at[pl.ds(0, count)]
        return remote(got, got, e_ssem.at[0], e_rsem.at[0], {"feat": near})

    def drain_all(count):
        for drain in (pair_drain, far_drain, res_drain):
            drain()
        for h in range(PARTS + 1):
            g_all(h, 0, count).wait_send()

    @pl.when(leads)
    def _():
        state_copy.wait_recv()
        energy = state_ref[0, own + 8:, :LANES] + state_ref[1, own + 8:, :LANES]
        totals = []
        for h in range(PARTS):
            if h == PARTS - 1:
                loss = total_of(PARTS, 0) + total_of(PARTS, 1)
                loss = jnp.concatenate([loss, pltpu.roll(loss, LANES - 2 * chains, 1)], axis=0)
                energy = energy + loss + pltpu.roll(loss, LANES - chains, 1)
            cols = slice(h * part_width, (h + 1) * part_width)
            squares = []
            for side in range(2):
                total = total_of(h, side)
                if side:
                    tot_send[h] = total
                else:
                    totals.append(total)
                t = state_ref[side, :own, cols] - 0.5 * step_size * total
                squares.append(state_ref[side, own:own + 1, cols] * t * t)
            both = jnp.dot(
                stacked(squares[0] + squares[1]), gather_ref[cols, :], preferred_element_type=F32
            )
            energy = energy + both[:own] + both[own:]
        esend[...] = energy
        for i in range(1, nf):
            e_copy(i).start()
        tot_copy.start()
        erecv[feat // 2] = esend[...]
        write(totals)
        drain_all(n - 1)
        for side in range(2):
            sent(side).wait_send()
        tot_copy.wait_send()
        sent_e = state_ref.at[1, pl.ds(0, 8 * (nf - 1)), pl.ds(0, own * LANES // 8)]
        remote(sent_e, sent_e, e_ssem.at[0], e_rsem.at[0], {"feat": near}).wait_send()
        if nf > 2:
            e_all(nf // 2 - 1).wait_recv()

    @pl.when(follows)
    def _():
        tot_copy.wait_recv()
        write([tot_recv[h] for h in range(PARTS)])
        drain_all(n)
        hand_all.wait_send()
        state_copy.wait_send()
        e_all(nf // 2).wait_recv()

    e = erecv[0]
    for i in range(1, nf // 2):
        e = e + erecv[i]
    energy_ref[...] = e[:, :chains]


def finish(*refs):
    sem = refs[8]
    copies = [pltpu.make_async_copy(refs[i], refs[4 + i], sem.at[i]) for i in range(4)]
    for c in copies:
        c.start()
    for c in copies:
        c.wait()


def body(observations, labels, tile_live, tile_group, position, momentum, gradient, prior_mean, prior_prec, inv_mass):
    n, nf = lax.axis_size("dp"), lax.axis_size("feat")
    tiles, quarter, row_count = observations.shape
    own, width = position.shape
    chains = width // quarter
    pack = LANES // quarter
    half_rows = tiles * chains // 2
    anywhere = pl.BlockSpec(memory_space=pl.ANY)
    units = PARTS * CHUNKS
    dma = pltpu.SemaphoreType.DMA
    block = pltpu.VMEM((own, width), F32)
    results = pl.pallas_call(
        functools.partial(kernel, n, nf, chains, quarter),
        out_shape=(block, block, block, pltpu.VMEM((own, chains), F32)),
        in_specs=[anywhere] * 10,
        out_specs=(pl.BlockSpec(memory_space=pltpu.VMEM),) * 4,
        scratch_shapes=[
            pltpu.VMEM((tiles, row_count), jnp.int32),
            pltpu.VMEM((1, tiles), jnp.int32),
            pltpu.VMEM((1, tiles), jnp.int32),
            pltpu.VMEM((own, width), F32),
            pltpu.VMEM((own, width), F32),
            pltpu.VMEM((own, width), F32),
            pltpu.VMEM((1, width), F32),
            pltpu.VMEM((2, quarter), F32),
            pltpu.VMEM((tiles, row_count), F32),
            pltpu.VMEM((2, width), F32),
            pltpu.VMEM((tiles // pack // 2, 2 * LANES, row_count), BF16),
            pltpu.VMEM((width, width), BF16),
            pltpu.VMEM((width, width), BF16),
            pltpu.VMEM((PARTS, own, width // PARTS), BF16),
            pltpu.VMEM((2, PARTS, n * own, width // PARTS), BF16),
            pltpu.VMEM((own, width), F32),
            pltpu.VMEM((2, 2 * own + 8, width), F32),
            pltpu.VMEM((PARTS, own, width // PARTS), F32),
            pltpu.VMEM((PARTS, own, width // PARTS), F32),
            pltpu.VMEM((width, LANES), BF16),
            pltpu.VMEM((tiles, n * own), BF16),
            pltpu.VMEM((2, n * own, tiles), BF16),
            pltpu.VMEM((2, n * own, tiles - tiles // CHUNKS), BF16),
            pltpu.VMEM((2, n * own, tiles // CHUNKS), BF16),
            pltpu.VMEM((PARTS, tiles // pack // 2, 2 * pack * chains // PARTS, 2 * LANES), BF16),
            pltpu.VMEM((half_rows, row_count), F32),
            pltpu.VMEM((half_rows, row_count), F32),
            pltpu.VMEM((half_rows, row_count), F32),
            pltpu.VMEM((half_rows, row_count), BF16),
            pltpu.VMEM((half_rows, row_count), BF16),
            pltpu.VMEM((half_rows, row_count), BF16),
            pltpu.VMEM((half_rows, row_count), BF16),
            pltpu.VMEM((tiles, LANES), F32),
            pltpu.VMEM((chains, tiles, LANES), F32),
            pltpu.VMEM((n * own, width // PARTS), F32),
            pltpu.VMEM((n * own, width // PARTS), BF16),
            pltpu.VMEM((n * own, width // PARTS), BF16),
            pltpu.VMEM((n, own // 2, LANES), BF16),
            pltpu.VMEM((2, n, own, width // PARTS), BF16),
            pltpu.VMEM((2, n, own, width // PARTS), BF16),
            pltpu.VMEM((2, n, own // 2, LANES), BF16),
            pltpu.VMEM((own, LANES), F32),
            pltpu.VMEM((nf // 2, own, LANES), F32),
            dma((10,)),
            dma((1,)), dma((PARTS,)), dma((PARTS, max(n, units))),
            dma((units,)), dma((units,)), dma((2, PARTS + 1)), dma((1,)), dma((1,)),
        ],
        compiler_params=pltpu.CompilerParams(collective_id=0, has_side_effects=True),
    )(
        observations.reshape(tiles // pack // 2, 2 * LANES, row_count),
        labels, tile_live.reshape(1, tiles), tile_group.reshape(1, tiles),
        position, momentum, gradient,
        prior_mean.reshape(1, width), prior_prec.reshape(1, quarter), inv_mass.reshape(1, quarter),
    )
    return tuple(pl.pallas_call(
        finish,
        out_shape=tuple(jax.ShapeDtypeStruct(x.shape, x.dtype) for x in results),
        in_specs=[pl.BlockSpec(memory_space=pltpu.VMEM)] * 4,
        out_specs=(anywhere,) * 4,
        scratch_shapes=[dma((4,))],
    )(*(pltpu.with_memory_space_constraint(x, pltpu.VMEM) for x in results)))


def solution(mesh):
    placed = (
        P("dp", "feat", None),
        P("dp", None),
        P("dp"),
        P("dp"),
        P("dp", "feat"),
        P("dp", "feat"),
        P("dp", "feat"),
        P("feat"),
        P("feat"),
        P("feat"),
    )
    return jax.shard_map(
        body,
        mesh=mesh,
        in_specs=placed,
        out_specs=(P("dp", "feat"), P("dp", "feat"), P("dp", "feat"), P("dp", None)),
        check_vma=False,
    )
```

```python
import functools
import jax
import jax.numpy as jnp
from jax import lax
from jax.experimental import pallas as pl
from jax.experimental.pallas import tpu as pltpu
from jax.sharding import PartitionSpec as P

step_size = 0.1
LANES = 128
PARTS = 2
CHUNKS = 4
MESH = pl.DeviceIdType.MESH
BF16 = jnp.bfloat16
F32 = jnp.float32


def iota(shape, dim):
    return lax.broadcasted_iota(jnp.int32, shape, dim)


def split(x):
    hi = x.astype(BF16)
    return hi, (x - hi.astype(F32)).astype(BF16)


def nt_dot(a, b):
    return lax.dot_general(a, b, (((1,), (1,)), ((), ())), preferred_element_type=F32)


def kernel(
    n, nf, chains, quarter,
    obs_hbm, lab_hbm, live_hbm, grp_hbm, pos_hbm, mom_hbm, grad_hbm, mean_hbm, prec_hbm, mass_hbm,
    newpos_ref, newmom_ref, newgrad_ref, energy_ref,
    lab_in, live_ref, grp_ref, pos_ref, mom_ref, grad_ref, mean_ref, pair_ref,
    lab_ref, par_ref, obs, perm, back, hand, wall, half_ref, state_ref, tot_send, tot_recv, gather_ref, hot_ref, sum_ref, most_ref, last_ref, lhs, mine, pair_send, pair_recv,
    far_send, far_recv, res_own, res_recv, nll_ref, dmat, acc, gsend0, gsend1, nsend, grecv0, grecv1, nrecv, esend, erecv,
    in_sem, h_rsem, w_rsem, t_sem, p_rsem, f_rsem, g_rsem, e_rsem, s_rsem,
):
    h_ssem, w_ssem, p_ssem, f_ssem = (in_sem.at[i:j] for i, j in ((0, 1), (1, 3), (3, 4), (4, 5)))
    r_ssem, g_ssem, e_ssem = (in_sem.at[i:j] for i, j in ((5, 6), (6, 9), (9, 10)))
    r_rsem = t_sem.at[0]
    me = lax.axis_index("dp")
    feat = lax.axis_index("feat")
    tiles = lab_ref.shape[0]
    own, width = pos_ref.shape
    pack = LANES // quarter
    part_chains = chains // PARTS
    part_width = width // PARTS
    octet = 2 * pack
    orows = octet * part_chains
    half_octets = tiles // octet // 2
    chunk_octets = half_octets // CHUNKS
    chunk_tiles = chunk_octets * octet
    crows = chunk_octets * orows
    groups = n * own
    bit = feat % 2
    near = feat + 1 - 2 * bit
    far = (feat + nf // 2) % nf

    barrier = pltpu.get_barrier_semaphore()

    def above(body):
        def step(i, carry):
            body(n - 1 - i)
            return carry

        lax.fori_loop(0, n - 1 - me, step, 0)

    def below(body):
        def step(d, carry):
            body(d)
            return carry

        lax.fori_loop(0, me, step, 0)

    def others(body):
        above(body)
        below(body)

    def greet(d):
        pl.semaphore_signal(barrier, inc=1, device_id={"dp": d}, device_id_type=MESH)

    leads = bit == 1
    follows = bit == 0

    @pl.when(leads)
    def _():
        below(greet)

    above(greet)
    for i in range(1, nf):
        pl.semaphore_signal(barrier, inc=1, device_id={"feat": (feat + i) % nf}, device_id_type=MESH)

    sources = [
        (mass_hbm, pair_ref.at[1:2]), (prec_hbm, pair_ref.at[0:1]),
        (mom_hbm, mom_ref), (grad_hbm, grad_ref), (pos_hbm, pos_ref), (mean_hbm, mean_ref),
        (grp_hbm, grp_ref), (live_hbm, live_ref), (lab_hbm, lab_in), (obs_hbm, obs),
    ]
    fetches = [pltpu.make_async_copy(a, b, in_sem.at[i]) for i, (a, b) in enumerate(sources)]
    for f in fetches:
        f.start()

    spread = (iota((quarter, width), 0) == iota((quarter, width), 1) // chains).astype(F32)
    r, c = iota((width, width), 0), iota((width, width), 1)
    perm[...] = jnp.where(
        (r % chains == c // quarter) & (r // chains == c % quarter), 1.0, 0.0
    ).astype(BF16)
    for f in fetches[:5]:
        f.wait()
    par_ref[...] = jnp.dot(
        pair_ref[...], spread, precision=lax.Precision.HIGHEST, preferred_element_type=F32
    )
    half = mom_ref[...] - 0.5 * step_size * grad_ref[...]
    half_ref[...] = half
    moved = pos_ref[...] + step_size * par_ref[1:2, :] * half
    newpos_ref[...] = moved
    coeff = jnp.dot(moved.astype(BF16), perm[...], preferred_element_type=F32).astype(BF16)

    back[...] = jnp.where(
        (c % chains == r // quarter) & (c // chains == r % quarter), 1.0, 0.0
    ).astype(BF16)

    def block(d):
        return pl.ds(pl.multiple_of(d * own, own), own)

    for h in range(PARTS):
        hand[h] = coeff[:, h * part_width:(h + 1) * part_width]

    for h in range(PARTS):
        wall[0, h, block(me), :] = hand[h]
    pl.semaphore_wait(barrier, me + (n - 1 - me) * bit + nf - 1)

    def remote(src, dst, ssem, rsem, to):
        return pltpu.make_async_remote_copy(
            src_ref=src, dst_ref=dst, send_sem=ssem, recv_sem=rsem,
            device_id=to, device_id_type=MESH,
        )

    def hand_copy(h):
        return remote(
            hand.at[h], wall.at[1, h, block(me)], h_ssem.at[0], h_rsem.at[0], {"feat": near}
        )

    def w_copy(h, to, ssem):
        rows = wall.at[0, h, block(me)]
        return remote(rows, rows, ssem, w_rsem.at[h], {"dp": to})

    def t_copy(h, d, to):
        rows = wall.at[1, h, block(d)]
        return remote(rows, rows, w_ssem.at[1], t_sem.at[h, d], {"dp": to})

    def w_all(h):
        blocks = wall.at[0, h, pl.ds(0, (n - 1) * own)]
        return remote(blocks, blocks, w_ssem.at[0], w_rsem.at[h], {"dp": (me + 1) % n})

    def sent(side):
        blocks = wall.at[side, :, pl.ds(0, (n - 1) * own)]
        return remote(blocks, blocks, w_ssem.at[side], w_rsem.at[0], {"dp": (me + 1) % n})

    def pass_on(h, d):
        return remote(
            wall.at[1, h, block(d)], wall.at[0, h, block(d)], w_ssem.at[1], w_rsem.at[h],
            {"feat": near},
        )

    hand_all = remote(hand, hand, h_ssem.at[0], h_rsem.at[0], {"feat": near})

    @pl.when(jnp.logical_not(leads))
    def _():
        for h in range(PARTS):
            hand_copy(h).start()
        for h in range(PARTS):
            below(lambda d: w_copy(h, d, t_sem.at[h, d]).start())

    def send_both(h, d):
        t_copy(h, me, d).start()
        w_copy(h, d, w_ssem.at[0]).start()

    @pl.when(leads)
    def _():
        for h in range(PARTS):
            below(lambda d: w_copy(h, d, w_ssem.at[0]).start())
        hand_all.wait_recv()
        for h in range(PARTS):
            above(lambda d: send_both(h, d))

    square = iota((tiles, tiles), 0) == iota((tiles, tiles), 1)

    def column(row):
        return jnp.sum(jnp.where(square, row.astype(F32), 0.0), axis=1, keepdims=True)

    for f in fetches[5:9]:
        f.wait()
    hot_ref[...] = (
        iota((tiles, groups), 1).astype(F32) == column(grp_ref[...])
    ).astype(F32).astype(BF16)
    member = (iota((groups, tiles), 0) == grp_ref[...]).astype(F32).astype(BF16)
    for i in range(2):
        side = member[:, i * (tiles // 2):(i + 1) * (tiles // 2)]
        sum_ref[i] = jnp.concatenate([side, side], axis=1)
        most_ref[i] = jnp.concatenate([side[:, :-chunk_tiles]] * 2, axis=1)
        last_ref[i] = jnp.concatenate([side[:, -chunk_tiles:]] * 2, axis=1)
    lab_ref[...] = jnp.where(
        iota(lab_ref.shape, 1).astype(F32) < column(live_ref[...]), lab_in[...].astype(F32), -1.0
    )
    nll_ref[...] = jnp.zeros_like(nll_ref)
    offset = newpos_ref[...] - mean_ref[...]
    force = par_ref[0:1, :] * offset
    drift = half_ref[...] - 0.5 * step_size * force
    high, rest = split(drift)
    low = (drift - high.astype(F32) - rest.astype(F32)).astype(BF16)
    packed = jnp.dot(
        jnp.concatenate([high, rest, low], axis=0), perm[...], preferred_element_type=F32
    )
    state_ref[0, :own, :] = packed[:own] + packed[own:2 * own] + packed[2 * own:]
    lane_mass = jnp.dot(
        pair_ref[...], (iota((quarter, width), 0) == iota((quarter, width), 1) % quarter).astype(F32),
        precision=lax.Precision.HIGHEST, preferred_element_type=F32,
    )[1:2, :]
    state_ref[0, own:own + 8, :] = jnp.broadcast_to(0.5 * lane_mass, (8, width))
    gather_ref[...] = (
        iota((width, LANES), 0) // quarter == iota((width, LANES), 1)
    ).astype(F32).astype(BF16)
    prior = 0.5 * force * offset
    e0 = prior[:, :LANES]
    for m in range(1, width // LANES):
        e0 = e0 + prior[:, m * LANES:(m + 1) * LANES]
    shift = LANES // 2
    while shift >= chains:
        e0 = e0 + pltpu.roll(e0, shift, 1)
        shift //= 2
    state_ref[0, own + 8:, :] = jnp.concatenate([e0] * (width // LANES), axis=1)
    fetches[9].wait()
    state_copy = remote(state_ref.at[0], state_ref.at[1], e_ssem.at[0], s_rsem.at[0], {"feat": near})
    pl.when(follows)(lambda: state_copy.start())

    half_tiles = tiles // 2
    row_t, lane_t = iota((tiles, LANES), 0), iota((tiles, LANES), 1)
    place = row_t % pack
    keep = lane_t // quarter == place
    sides = (keep & (row_t % octet < pack), keep & (row_t % octet >= pack))
    mine_first, near_first = bit * half_tiles, (1 - bit) * half_tiles

    def hand_over(h, d):
        t_copy(h, d, d).wait_recv()
        pass_on(h, d).start()

    def relay(h):
        @pl.when(leads)
        def _():
            below(lambda d: hand_over(h, d))

    def pick(h):
        picked = jnp.dot(hot_ref[...], wall[0, h], preferred_element_type=F32)
        for m in range(part_width // LANES):
            x = picked[:, m * LANES:(m + 1) * LANES]
            turned = [x] + [pltpu.roll(x, s * quarter, 1) for s in range(1, pack)]
            spots = []
            for j in range(pack):
                y = turned[0]
                for s in range(1, pack):
                    y = jnp.where((place + pack - j) % pack == s, turned[s], y)
                spots.append(y)
            for j in range(0, pack, 2):
                at = (m * pack + j) * octet
                for i, side in enumerate(sides):
                    two = jnp.concatenate([
                        jnp.where(side, y, 0.0).reshape(tiles // octet, octet, LANES)
                        for y in spots[j:j + 2]
                    ], axis=1)
                    lhs[h, :, at:at + 2 * octet, i * LANES:(i + 1) * LANES] = two.astype(BF16)

    def logits(h, first_octet, dst, base):
        for i in range(chunk_octets):
            o = first_octet + i
            dst[base + i * orows:base + (i + 1) * orows, :] = jnp.dot(
                lhs[h, o], obs[o], preferred_element_type=F32
            ).astype(dst.dtype)

    units = PARTS * CHUNKS

    def rows(u):
        return pl.ds(u * crows, crows)

    def exchange(src, dst, ssem, rsem, to):
        def copy(u):
            at = pl.ds(u * crows, crows)
            return remote(src.at[at], dst.at[at], ssem.at[0], rsem.at[u], {"feat": to})

        def drain():
            pltpu.make_async_remote_copy(
                src_ref=src, dst_ref=dst, send_sem=ssem.at[0], recv_sem=rsem.at[0],
                device_id={"feat": to}, device_id_type=MESH,
            ).wait_send()

        return copy, drain

    pair_copy, pair_drain = exchange(pair_send, pair_recv, p_ssem, p_rsem, near)
    far_copy, far_drain = exchange(far_send, far_recv, f_ssem, f_rsem, far)
    res_copy, res_drain = exchange(res_own, res_recv, r_ssem, r_rsem, near)

    for h in range(PARTS):
        if h == 0:
            relay(h)

        w_all(h).wait_recv()
        pl.when(jnp.logical_not(leads))(
            lambda: below(lambda d: w_copy(h, d, t_sem.at[h, d]).wait_send())
        )
        pick(h)
        mark = h * CHUNKS
        for k in range(CHUNKS):
            logits(h, (1 - bit) * half_octets + k * chunk_octets, pair_send, (mark + k) * crows)
        for u in range(mark, mark + CHUNKS):
            pair_copy(u).start()
        if h + 1 < PARTS:
            relay(h + 1)
        for k in range(CHUNKS):
            logits(h, bit * half_octets + k * chunk_octets, mine, (mark + k) * crows)
        for u in range(mark, mark + CHUNKS):
            pair_copy(u).wait_recv()
            total = mine[rows(u), :] + pair_recv[rows(u), :].astype(F32)
            mine[rows(u), :] = total
            far_send[rows(u), :] = total.astype(BF16)
            far_copy(u).start()

    spot = iota((orows, LANES), 0) % octet
    diag = tuple(spot == iota((orows, LANES), 1) // quarter + i * pack for i in range(2))

    def grads(h, first_octet, src, base):
        for i in range(chunk_octets):
            o = first_octet + i
            g = nt_dot(src[base + i * orows:base + (i + 1) * orows, :], obs[o])
            g = jnp.where(diag[0], g[:, :LANES], jnp.where(diag[1], g[:, LANES:], 0.0))
            tile = pl.ds(pl.multiple_of(o * octet, octet), octet)
            dmat[h * part_chains:(h + 1) * part_chains, tile, :] = g.reshape(part_chains, octet, LANES)

    def residual(u):
        h, k = divmod(u, CHUNKS)
        z = mine[rows(u), :] + far_recv[rows(u), :].astype(F32)
        first = pl.multiple_of((bit * half_octets + k * chunk_octets) * octet, chunk_tiles)
        lab = lab_ref[pl.ds(first, chunk_tiles), :]
        lab = lab.reshape(chunk_octets, 1, octet, LANES)
        lab = jnp.broadcast_to(lab, (chunk_octets, part_chains, octet, LANES)).reshape(crows, LANES)
        live = lab >= 0.0
        e = jnp.exp(-jnp.abs(z))
        inv = 1.0 / (1.0 + e)
        sig = jnp.where(z >= 0.0, inv, e * inv)
        res_own[rows(u), :] = jnp.where(live, sig - lab, 0.0).astype(BF16)
        res_copy(u).start()
        v = jnp.where(live, jnp.maximum(z, 0.0) + jnp.log(1.0 + e) - lab * z, 0.0)
        s = jnp.sum(v, axis=1, keepdims=True) * (2.0 / nf)
        at = iota((crows, LANES), 0) // octet % part_chains + h * part_chains == iota((crows, LANES), 1)
        s = jnp.where(at, s, 0.0).reshape(chunk_octets, part_chains, octet, LANES)
        nll_ref[pl.ds(first, chunk_tiles), :] += jnp.sum(s, axis=1).reshape(chunk_tiles, LANES)

    def mine_grads(u):
        h, k = divmod(u, CHUNKS)
        grads(h, bit * half_octets + k * chunk_octets, res_own, u * crows)

    def near_grads(u):
        h, k = divmod(u, CHUNKS)
        grads(h, (1 - bit) * half_octets + k * chunk_octets, res_recv, u * crows)

    seg_groups = min(groups, LANES)
    lane_g = iota((half_tiles, LANES), 1) // quarter
    blocks = part_width // LANES
    sums = ((gsend0, grecv0), (gsend1, grecv1), (nsend, nrecv))

    def stacked(d):
        return jnp.concatenate(split(d), axis=0)

    def fold(xs, width):
        if len(xs) == 1:
            return xs[0]
        half = len(xs) // 2
        shift = half * width
        low = lane_g[:xs[0].shape[0]] % len(xs) < half
        pairs = []
        for a, b in zip(xs[:half], xs[half:]):
            other = jnp.where(low, b, a)
            if len(xs) == pack:
                moved = pltpu.roll(other, shift, 1)
            else:
                moved = jnp.where(
                    low, pltpu.roll(other, LANES - shift, 1), pltpu.roll(other, shift, 1)
                )
            pairs.append(jnp.where(low, a, b) + moved)
        return fold(pairs, width)

    def compact(h, first, start=0, count=None):
        count = count or half_tiles
        out = []
        for m in range(blocks):
            xs = []
            for j in range(pack):
                tile = pl.ds(pl.multiple_of(first + start, octet), count)
                xs.append(dmat[h * part_chains + m * pack + j, tile, :])
            out.append(fold(xs, quarter))
        return stacked(jnp.concatenate(out, axis=1))

    def over_groups(body):
        def run(gc, carry):
            body(pl.ds(pl.multiple_of(gc * seg_groups, seg_groups), seg_groups))
            return carry

        if groups == seg_groups:
            body(pl.ds(0, groups))
        else:
            lax.fori_loop(0, groups // seg_groups, run, 0)

    def member_dot(side, out, rhs):
        return jnp.dot(sum_ref[side, out, :], rhs, preferred_element_type=F32)

    most = half_tiles - chunk_tiles

    def start_half(h):
        rhs = compact(h, mine_first)
        rest = compact(h, near_first, 0, most)
        def body(out):
            acc[out, :] = member_dot(bit, out, rhs) + jnp.dot(
                most_ref[1 - bit, out, :], rest, preferred_element_type=F32
            )
        over_groups(body)

    def whole(h):
        rhs = compact(h, mine_first), compact(h, near_first)

        def body(out):
            sums[h][0][out, :] = (
                member_dot(bit, out, rhs[0]) + member_dot(1 - bit, out, rhs[1])
            ).astype(BF16)

        over_groups(body)

    def finish_half(h):
        rhs = compact(h, near_first, most, chunk_tiles)

        def body(out):
            sums[h][0][out, :] = (acc[out, :] + jnp.dot(last_ref[1 - bit, out, :], rhs, preferred_element_type=F32)).astype(BF16)

        over_groups(body)

    def g_copy(h, to):
        src = nsend.at[to] if h == PARTS else sums[h][0].at[block(to)]
        return remote(
            src, sums[h][1].at[1 - bit, me], g_ssem.at[h], g_rsem.at[1 - bit, h],
            {"dp": to, "feat": feat + 1 - bit},
        )

    def g_all(h, side, count):
        got = sums[h][1].at[side, pl.ds(0, count)]
        return remote(got, got, g_ssem.at[h], g_rsem.at[side, h], {"feat": near})

    def send_sums(h):
        below(lambda d: g_copy(h, d).start())
        above(lambda d: g_copy(h, d).start())

        @pl.when(leads)
        def _():
            sums[h][1][0, me] = nsend[me] if h == PARTS else sums[h][0][block(me), :]

        pl.when(follows)(lambda: g_copy(h, me).start())

    def loss_sums():
        nll = stacked(nll_ref[pl.ds(pl.multiple_of(mine_first, half_tiles), half_tiles), :])

        def body(out):
            hi, lo = split(member_dot(bit, out, nll))
            loss = hi.astype(F32) + pltpu.roll(lo.astype(F32), chains, 1)
            loss = loss.reshape(seg_groups // own, 2, own // 2, LANES)
            loss = loss[:, 0].reshape(-1, LANES) + pltpu.roll(
                loss[:, 1].reshape(-1, LANES), 2 * chains, 1
            )
            owners = pl.ds(out.start // own, seg_groups // own)
            nsend[owners] = loss.reshape(-1, own // 2, LANES).astype(BF16)

        over_groups(body)
        send_sums(PARTS)

    lag = 2

    def near_step(u):
        res_copy(u).wait_recv()
        near_grads(u)

    for u in range(units):
        if u == units - 1:
            near_step(u - lag)
        far_copy(u).wait_recv()
        if lag <= u < units - 1:
            res_copy(u - lag).wait_recv()
        residual(u)
        if u == units - 1:
            loss_sums()
        mine_grads(u)
        if lag <= u < units - 1:
            near_grads(u - lag)
            h, k = divmod(u - lag, CHUNKS)
            if k == CHUNKS - 1:
                whole(h)
                send_sums(h)
    near_step(units - 2)
    start_half(PARTS - 1)
    near_step(units - 1)
    finish_half(PARTS - 1)
    send_sums(PARTS - 1)

    def total_of(h, side):
        g_all(h, side, n - 1 + side).wait_recv()
        return jnp.sum(sums[h][1][side].astype(F32), axis=0)

    def natural(packed, h):
        parts = jnp.concatenate(split(packed), axis=0)
        both = jnp.dot(
            parts, back[h * part_width:(h + 1) * part_width, :], preferred_element_type=F32
        )
        return both[:own] + both[own:]

    def write(totals):
        new_gradient = par_ref[0:1, :] * (newpos_ref[...] - mean_ref[...])
        for h in range(PARTS):
            new_gradient = new_gradient + natural(totals[h], h)
        newgrad_ref[...] = new_gradient
        newmom_ref[...] = half_ref[...] - 0.5 * step_size * new_gradient

    tot_copy = remote(tot_send, tot_recv, h_ssem.at[0], s_rsem.at[0], {"feat": near})

    def e_copy(i):
        return remote(
            esend, erecv.at[feat // 2], e_ssem.at[0], e_rsem.at[0], {"feat": (feat + i) % nf}
        )

    def e_all(count):
        got = erecv.at[pl.ds(0, count)]
        return remote(got, got, e_ssem.at[0], e_rsem.at[0], {"feat": near})

    def drain_all(count):
        for drain in (pair_drain, far_drain, res_drain):
            drain()
        for h in range(PARTS + 1):
            g_all(h, 0, count).wait_send()

    @pl.when(leads)
    def _():
        state_copy.wait_recv()
        energy = state_ref[0, own + 8:, :LANES] + state_ref[1, own + 8:, :LANES]
        totals = []
        for h in range(PARTS):
            if h == PARTS - 1:
                loss = total_of(PARTS, 0) + total_of(PARTS, 1)
                loss = jnp.concatenate([loss, pltpu.roll(loss, LANES - 2 * chains, 1)], axis=0)
                energy = energy + loss + pltpu.roll(loss, LANES - chains, 1)
            cols = slice(h * part_width, (h + 1) * part_width)
            squares = []
            for side in range(2):
                total = total_of(h, side)
                if side:
                    tot_send[h] = total
                else:
                    totals.append(total)
                t = state_ref[side, :own, cols] - 0.5 * step_size * total
                squares.append(state_ref[side, own:own + 1, cols] * t * t)
            both = jnp.dot(
                stacked(squares[0] + squares[1]), gather_ref[cols, :], preferred_element_type=F32
            )
            energy = energy + both[:own] + both[own:]
        esend[...] = energy
        for i in range(1, nf):
            e_copy(i).start()
        tot_copy.start()
        erecv[feat // 2] = esend[...]
        write(totals)
        drain_all(n - 1)
        for side in range(2):
            sent(side).wait_send()
        tot_copy.wait_send()
        sent_e = state_ref.at[1, pl.ds(0, 8 * (nf - 1)), pl.ds(0, own * LANES // 8)]
        remote(sent_e, sent_e, e_ssem.at[0], e_rsem.at[0], {"feat": near}).wait_send()
        if nf > 2:
            e_all(nf // 2 - 1).wait_recv()

    @pl.when(follows)
    def _():
        tot_copy.wait_recv()
        write([tot_recv[h] for h in range(PARTS)])
        drain_all(n)
        hand_all.wait_send()
        state_copy.wait_send()
        e_all(nf // 2).wait_recv()

    e = erecv[0]
    for i in range(1, nf // 2):
        e = e + erecv[i]
    energy_ref[...] = e[:, :chains]


def finish(*refs):
    sem = refs[8]
    copies = [pltpu.make_async_copy(refs[i], refs[4 + i], sem.at[i]) for i in range(4)]
    for c in copies:
        c.start()
    for c in copies:
        c.wait()


def body(observations, labels, tile_live, tile_group, position, momentum, gradient, prior_mean, prior_prec, inv_mass):
    n, nf = lax.axis_size("dp"), lax.axis_size("feat")
    tiles, quarter, row_count = observations.shape
    own, width = position.shape
    chains = width // quarter
    pack = LANES // quarter
    half_rows = tiles * chains // 2
    anywhere = pl.BlockSpec(memory_space=pl.ANY)
    units = PARTS * CHUNKS
    dma = pltpu.SemaphoreType.DMA
    block = pltpu.VMEM((own, width), F32)
    results = pl.pallas_call(
        functools.partial(kernel, n, nf, chains, quarter),
        out_shape=(block, block, block, pltpu.VMEM((own, chains), F32)),
        in_specs=[anywhere] * 10,
        out_specs=(pl.BlockSpec(memory_space=pltpu.VMEM),) * 4,
        scratch_shapes=[
            pltpu.VMEM((tiles, row_count), jnp.int32),
            pltpu.VMEM((1, tiles), jnp.int32),
            pltpu.VMEM((1, tiles), jnp.int32),
            pltpu.VMEM((own, width), F32),
            pltpu.VMEM((own, width), F32),
            pltpu.VMEM((own, width), F32),
            pltpu.VMEM((1, width), F32),
            pltpu.VMEM((2, quarter), F32),
            pltpu.VMEM((tiles, row_count), F32),
            pltpu.VMEM((2, width), F32),
            pltpu.VMEM((tiles // pack // 2, 2 * LANES, row_count), BF16),
            pltpu.VMEM((width, width), BF16),
            pltpu.VMEM((width, width), BF16),
            pltpu.VMEM((PARTS, own, width // PARTS), BF16),
            pltpu.VMEM((2, PARTS, n * own, width // PARTS), BF16),
            pltpu.VMEM((own, width), F32),
            pltpu.VMEM((2, 2 * own + 8, width), F32),
            pltpu.VMEM((PARTS, own, width // PARTS), F32),
            pltpu.VMEM((PARTS, own, width // PARTS), F32),
            pltpu.VMEM((width, LANES), BF16),
            pltpu.VMEM((tiles, n * own), BF16),
            pltpu.VMEM((2, n * own, tiles), BF16),
            pltpu.VMEM((2, n * own, tiles - tiles // CHUNKS), BF16),
            pltpu.VMEM((2, n * own, tiles // CHUNKS), BF16),
            pltpu.VMEM((PARTS, tiles // pack // 2, 2 * pack * chains // PARTS, 2 * LANES), BF16),
            pltpu.VMEM((half_rows, row_count), F32),
            pltpu.VMEM((half_rows, row_count), F32),
            pltpu.VMEM((half_rows, row_count), F32),
            pltpu.VMEM((half_rows, row_count), BF16),
            pltpu.VMEM((half_rows, row_count), BF16),
            pltpu.VMEM((half_rows, row_count), BF16),
            pltpu.VMEM((half_rows, row_count), BF16),
            pltpu.VMEM((tiles, LANES), F32),
            pltpu.VMEM((chains, tiles, LANES), F32),
            pltpu.VMEM((n * own, width // PARTS), F32),
            pltpu.VMEM((n * own, width // PARTS), BF16),
            pltpu.VMEM((n * own, width // PARTS), BF16),
            pltpu.VMEM((n, own // 2, LANES), BF16),
            pltpu.VMEM((2, n, own, width // PARTS), BF16),
            pltpu.VMEM((2, n, own, width // PARTS), BF16),
            pltpu.VMEM((2, n, own // 2, LANES), BF16),
            pltpu.VMEM((own, LANES), F32),
            pltpu.VMEM((nf // 2, own, LANES), F32),
            dma((10,)),
            dma((1,)), dma((PARTS,)), dma((PARTS, max(n, units))),
            dma((units,)), dma((units,)), dma((2, PARTS + 1)), dma((1,)), dma((1,)),
        ],
        compiler_params=pltpu.CompilerParams(collective_id=0, has_side_effects=True),
    )(
        observations.reshape(tiles // pack // 2, 2 * LANES, row_count),
        labels, tile_live.reshape(1, tiles), tile_group.reshape(1, tiles),
        position, momentum, gradient,
        prior_mean.reshape(1, width), prior_prec.reshape(1, quarter), inv_mass.reshape(1, quarter),
    )
    return tuple(pl.pallas_call(
        finish,
        out_shape=tuple(jax.ShapeDtypeStruct(x.shape, x.dtype) for x in results),
        in_specs=[pl.BlockSpec(memory_space=pltpu.VMEM)] * 4,
        out_specs=(anywhere,) * 4,
        scratch_shapes=[dma((4,))],
    )(*(pltpu.with_memory_space_constraint(x, pltpu.VMEM) for x in results)))


def solution(mesh):
    placed = (
        P("dp", "feat", None),
        P("dp", None),
        P("dp"),
        P("dp"),
        P("dp", "feat"),
        P("dp", "feat"),
        P("dp", "feat"),
        P("feat"),
        P("feat"),
        P("feat"),
    )
    return jax.shard_map(
        body,
        mesh=mesh,
        in_specs=placed,
        out_specs=(P("dp", "feat"), P("dp", "feat"), P("dp", "feat"), P("dp", None)),
        check_vma=False,
    )
```
